256 devices in a mesh: groups: 2 (over z), segment: 16 (over y, core), head: 8 (over x).
Axes of the slice: x: 8, y: 8, z: 2, core: 2. Of those that a mesh axis runs over, the one named last changes fastest.
The devices are a block of a 8x8x16 slice.
Arguments:
- token_ids: int32 [6, 256], P('groups'), parts along dimension 0, may hold values from 0 to 151935, as said below
- embed_table: bfloat16 [151936, 256], P(('segment', 'head')), may hold values from -6 to 6
- arriving: bfloat16 [32, 256, 256], P(('groups', 'segment')), parts along dimension 0, may hold values from -16 to 16
- returning: bfloat16 [32, 256, 256], P(('groups', 'segment')), parts along dimension 0, may hold values from -6 to 6
- stashed: bfloat16 [32, 3, 256, 256], P(('groups', 'segment')), parts along dimension 0, may hold values from -16 to 16
- seed_grad: bfloat16 [6, 256, 256], P('groups'), parts along dimension 0, may hold values from -6 to 6
- expand: bfloat16 [16, 256, 2048], P('segment'), may hold values from -0.375 to 0.375
- compress: bfloat16 [16, 2048, 256], P('segment'), may hold values from -0.125 to 0.125
- norm_gain: float32 [16, 2048], P('segment'), may hold values from 0.1 to 1.9
- w_query: bfloat16 [16, 2048, 4096], P('segment', None, 'head'), may hold values from -0.125 to 0.125
- key_weight: bfloat16 [16, 2048, 512], P('segment'), may hold values from -0.125 to 0.125
- value_weight: bfloat16 [16, 2048, 512], P('segment'), may hold values from -0.125 to 0.125
- w_out: bfloat16 [16, 4096, 2048], P('segment', 'head'), may hold values from -0.09375 to 0.09375
Outputs:
- sent_forward: bfloat16 [32, 3, 256, 256], P(('groups', 'segment'), None, 'head'), parts along dimension 0
- sent_backward: bfloat16 [32, 3, 256, 256], P(('groups', 'segment'), None, 'head'), parts along dimension 0
The draws below stay inside these ranges and needn't reach their ends.
There are 2 independent parts, one for each index of `groups`. The reference program is written for one: setup_inputs(seed, part) draws one part's arguments, and reference() takes and returns one part's arrays. A program takes and returns all parts, laid end to end along the dimension named above; an argument that names none is the same for every part. Nothing has to cross between parts.
Inputs may be any that keep to these rules, and one draw needn't show every extreme that they name: `token_ids`: every aligned block of 1187 ids is named by some token.
All inputs are finite; a program needn't handle non-finite values.
Results may differ from the reference program's by a relative error of at most 0.02.
Values may be sent and summed in bfloat16 or wider, within the bound.
No kernel may reach another device: no remote copies, remote signals or barrier semaphores. Data moves between devices by JAX's collectives and lax.ppermute only.
A program may use at most 128 MiB of HBM per device.

```python
import math
import jax
import jax.numpy as jnp
from jax import lax

MODEL_WIDTH = 2048
QUERY_HEADS = 32
KEY_VALUE_HEADS = 4
HEAD_SIZE = 128
RANK = 256
VOC_DEV = 1187
SPAN = 256
TICKS = 3
VOCAB = 151936
N_SEGMENT = 16
N_HEAD = 8


def draw_token_ids(key, part):
    token_count = TICKS * SPAN
    ranges = VOCAB // VOC_DEV
    share_rows = SPAN // N_HEAD
    drawn = jax.random.randint(jax.random.fold_in(key, 1), (token_count,), 0, VOCAB, dtype=jnp.int32)
    blocks = jnp.arange(ranges, dtype=jnp.int32)
    moved = (blocks + ranges - 1) % ranges
    share_of = moved % N_HEAD
    offset_of = moved // N_HEAD % share_rows
    tick_of = moved // SPAN
    places = (tick_of * SPAN + share_of * share_rows + offset_of).astype(jnp.int32)
    chosen = blocks * VOC_DEV + jax.random.randint(jax.random.fold_in(key, 3), (ranges,), 0, VOC_DEV, dtype=jnp.int32)
    return drawn.at[places].set(chosen).reshape(TICKS, SPAN).astype(jnp.int32)


def coefficient_rows(key, shape):
    normal_part = jax.random.normal(jax.random.fold_in(key, 21), shape, jnp.float32)
    return jnp.clip(normal_part, -16.0, 16.0).astype(jnp.bfloat16)


def draw_arriving(key, part):
    return coefficient_rows(key, (N_SEGMENT, SPAN, RANK))


def draw_stashed(key, part):
    return coefficient_rows(key, (N_SEGMENT, TICKS, SPAN, RANK))


def level_of(own_key, dims, split, least, high):
    def one(position, parts):
        steps = jax.random.uniform(jax.random.fold_in(jax.random.fold_in(own_key, 6), position), (parts,), jnp.float32, least / len(split), high / len(split))
        return jnp.repeat(jnp.exp(steps), dims[position] // parts).reshape((-1,) + (1,) * (len(dims) - position - 1))

    loudness = one(*split[0])
    for cut in split[1:]:
        loudness = loudness * one(*cut)
    return loudness


def bell_draw(key, extent, deviation, reach, cuts=(), kind=jnp.bfloat16):
    factor_of = level_of(key, extent, cuts, -0.22, 0.18) if cuts else 1.0
    values = jax.random.normal(key, extent, jnp.float32) * deviation * factor_of
    return jnp.minimum(jnp.maximum(values, -reach), reach).astype(kind)


def setup_inputs(seed: int = 0, part: int = 0) -> dict:
    streams_of = jax.random.split(jax.random.key(seed), 14)
    part_splits = jax.random.split(jax.random.fold_in(streams_of[13], part), 14)
    return {
        "token_ids": draw_token_ids(jax.random.fold_in(jax.random.fold_in(streams_of[13], part), 71), part),
        "embed_table": bell_draw(streams_of[1], (VOCAB, RANK), 1.0, 6.0, ((0, 128),)),
        "arriving": draw_arriving(jax.random.fold_in(jax.random.fold_in(streams_of[13], part), 71), part),
        "returning": bell_draw(part_splits[3], (N_SEGMENT, SPAN, RANK), 1.0, 6.0, ((0, 16),)),
        "stashed": draw_stashed(jax.random.fold_in(jax.random.fold_in(streams_of[13], part), 71), part),
        "seed_grad": bell_draw(part_splits[5], (TICKS, SPAN, RANK), 1.0, 6.0),
        "expand": bell_draw(streams_of[6], (N_SEGMENT, RANK, MODEL_WIDTH), RANK ** -0.5, 0.375, ((0, 16),)),
        "compress": bell_draw(streams_of[7], (N_SEGMENT, MODEL_WIDTH, RANK), MODEL_WIDTH ** -0.5, 0.125, ((0, 16),)),
        "norm_gain": jnp.clip(1.0 + 0.18 * jax.random.normal(streams_of[8], (N_SEGMENT, MODEL_WIDTH), jnp.float32), 0.1, 1.9),
        "w_query": bell_draw(streams_of[9], (N_SEGMENT, MODEL_WIDTH, QUERY_HEADS * HEAD_SIZE), MODEL_WIDTH ** -0.5, 0.125, ((0, 16), (2, 8))),
        "key_weight": bell_draw(streams_of[10], (N_SEGMENT, MODEL_WIDTH, KEY_VALUE_HEADS * HEAD_SIZE), MODEL_WIDTH ** -0.5, 0.125, ((0, 16),)),
        "value_weight": bell_draw(streams_of[11], (N_SEGMENT, MODEL_WIDTH, KEY_VALUE_HEADS * HEAD_SIZE), MODEL_WIDTH ** -0.5, 0.125, ((0, 16),)),
        "w_out": bell_draw(streams_of[12], (N_SEGMENT, QUERY_HEADS * HEAD_SIZE, MODEL_WIDTH), (QUERY_HEADS * HEAD_SIZE) ** -0.5, 0.09375, ((0, 16), (1, 8))),
    }


EPS = 1e-06

def rms_scale(matrix):
    return lax.rsqrt(lax.optimization_barrier(jnp.mean(matrix * matrix, axis=-1, keepdims=True)) + EPS)

def widened(matrix):
    return lax.optimization_barrier(matrix).astype(jnp.float32)

def precise(former, latter):
    return jnp.dot(former, latter, precision=lax.Precision.HIGHEST)

def precise_back(former, latter):
    return lax.dot_general(former, latter, (((1,), (1,)), ((), ())), precision=lax.Precision.HIGHEST)

def narrow_back(former, latter):
    return lax.dot_general(former, latter, (((1,), (1,)), ((), ())), preferred_element_type=jnp.float32)

def norm_back(upstream_in, grad_hat):
    scaling = rms_scale(upstream_in)
    return scaling * grad_hat - upstream_in * scaling ** 3 * lax.optimization_barrier(jnp.mean(grad_hat * upstream_in, axis=-1, keepdims=True))

def section_inputs(coeffs, expand_here, gain_here, query_here, key_here, value_here):
    row_count = coeffs.shape[0]
    hidden = jnp.dot(coeffs, expand_here, preferred_element_type=jnp.float32)
    scaling = rms_scale(hidden)
    normed = (hidden * scaling * gain_here).astype(jnp.bfloat16)
    queries = jnp.dot(normed, query_here, preferred_element_type=jnp.float32).reshape(row_count, -1, HEAD_SIZE)
    key_rows = jnp.dot(normed, key_here, preferred_element_type=jnp.float32).reshape(row_count, -1, HEAD_SIZE)
    values = jnp.dot(normed, value_here, preferred_element_type=jnp.float32).astype(jnp.bfloat16).reshape(row_count, -1, HEAD_SIZE)
    q_hat = (queries * rms_scale(queries)).astype(jnp.bfloat16)
    k_hat = (key_rows * rms_scale(key_rows)).astype(jnp.bfloat16)
    return (hidden, scaling, queries, key_rows, q_hat, k_hat, values)

def probabilities(q_hat, k_hat):
    row_count, head_count, head_width = q_hat.shape
    kv_heads = k_hat.shape[1]
    grouped = widened(q_hat).reshape(row_count, kv_heads, head_count // kv_heads, head_width)
    scores = jnp.einsum('iknd,jkd->knij', grouped, widened(k_hat)) / math.sqrt(head_width)
    causal = jnp.arange(row_count)[None, :] <= jnp.arange(row_count)[:, None]
    weights = jnp.where(causal, jnp.exp(scores), 0.0)
    return weights / lax.optimization_barrier(jnp.sum(weights, axis=-1, keepdims=True))

def section_forward(coeffs, expand_here, gain_here, query_here, key_here, value_here, out_folded, basis_folded):
    hidden, scaling, queries, key_rows, q_hat, k_hat, values = section_inputs(coeffs, expand_here, gain_here, query_here, key_here, value_here)
    weights = probabilities(q_hat, k_hat)
    low_weights = widened(weights.astype(jnp.bfloat16))
    attended = jnp.einsum('knij,jkd->iknd', low_weights, widened(values))
    attended = attended.reshape(coeffs.shape[0], -1).astype(jnp.bfloat16)
    return jnp.dot(attended, out_folded, preferred_element_type=jnp.float32) + precise(widened(coeffs), basis_folded)

def section_backward(coeffs, grads, expand_here, gain_here, query_here, key_here, value_here, out_folded, basis_folded):
    row_count = coeffs.shape[0]
    hidden, scaling, queries, key_rows, q_hat, k_hat, values = section_inputs(coeffs, expand_here, gain_here, query_here, key_here, value_here)
    weights = probabilities(q_hat, k_hat)
    head_count = queries.shape[1]
    kv_heads = key_rows.shape[1]
    query_group_size = head_count // kv_heads
    grads_wide = widened(grads)
    grad_attended = narrow_back(grads, out_folded).astype(jnp.bfloat16)
    grad_attended = widened(grad_attended).reshape(row_count, kv_heads, query_group_size, HEAD_SIZE)
    grad_weights = jnp.einsum('iknd,jkd->knij', grad_attended, widened(values))
    grad_scores = weights * (grad_weights - lax.optimization_barrier(jnp.sum(grad_weights * weights, axis=-1, keepdims=True))) / math.sqrt(HEAD_SIZE)
    grad_scores = widened(grad_scores.astype(jnp.bfloat16))
    grouped = widened(q_hat).reshape(row_count, kv_heads, query_group_size, HEAD_SIZE)
    grad_qhat = jnp.einsum('knij,jkd->iknd', grad_scores, widened(k_hat)).reshape(row_count, head_count, HEAD_SIZE)
    grad_khat = jnp.einsum('knij,iknd->jkd', grad_scores, grouped)
    low_weights = widened(weights.astype(jnp.bfloat16))
    grad_values = jnp.einsum('knij,iknd->jkd', low_weights, grad_attended).reshape(row_count, -1).astype(jnp.bfloat16)
    grad_queries = norm_back(queries, grad_qhat).reshape(row_count, -1).astype(jnp.bfloat16)
    grad_keys = norm_back(key_rows, grad_khat).reshape(row_count, -1).astype(jnp.bfloat16)
    grad_normed = narrow_back(grad_queries, query_here) + narrow_back(grad_keys, key_here) + narrow_back(grad_values, value_here)
    weighted = grad_normed * gain_here
    grad_hidden = scaling * weighted - hidden * scaling ** 3 * lax.optimization_barrier(jnp.mean(weighted * hidden, axis=-1, keepdims=True))
    grad_hidden = grad_hidden.astype(jnp.bfloat16)
    return narrow_back(grad_hidden, expand_here) + precise_back(grads_wide, basis_folded)

def reference(token_ids, embed_table, arriving, returning, stashed, seed_grad, expand, compress, norm_gain, w_query, key_weight, value_weight, w_out):
    segment_count = arriving.shape[0]
    last_segment = segment_count - 1
    embedded = embed_table[token_ids]
    folded = []
    for segment_index in range(segment_count):
        basis_folded = jnp.dot(expand[segment_index], compress[segment_index], preferred_element_type=jnp.float32)
        out_folded = jnp.dot(w_out[segment_index], compress[segment_index], preferred_element_type=jnp.float32).astype(jnp.bfloat16)
        folded.append((basis_folded, out_folded))
    history = []
    forward_sent = []
    backward_sent = []
    for tick_index in range(TICKS):
        forward_in = []
        backward_in = []
        for segment_index in range(segment_count):
            if segment_index == 0:
                forward_in.append(embedded[tick_index])
            elif tick_index == 0:
                forward_in.append(arriving[segment_index])
            else:
                forward_in.append(forward_sent[tick_index - 1][segment_index - 1])
            if segment_index == last_segment:
                backward_in.append(seed_grad[tick_index])
            elif tick_index == 0:
                backward_in.append(returning[segment_index])
            else:
                backward_in.append(backward_sent[tick_index - 1][segment_index + 1])
        history.append(forward_in)
        forward_out = []
        backward_out = []
        for segment_index in range(segment_count):
            basis_folded, out_folded = folded[segment_index]
            weights_here = (expand[segment_index], norm_gain[segment_index], w_query[segment_index], key_weight[segment_index], value_weight[segment_index])
            forward_out.append(section_forward(forward_in[segment_index], *weights_here, out_folded, basis_folded).astype(jnp.bfloat16))
            source = tick_index - 2 * (last_segment - segment_index)
            if source >= 0:
                replay = history[source][segment_index]
            else:
                replay = stashed[segment_index, tick_index]
            backward_out.append(section_backward(replay, backward_in[segment_index], *weights_here, out_folded, basis_folded).astype(jnp.bfloat16))
        forward_sent.append(forward_out)
        backward_sent.append(backward_out)
    sent_forward = jnp.stack([jnp.stack(entries) for entries in forward_sent], axis=1)
    sent_backward = jnp.stack([jnp.stack(entries) for entries in backward_sent], axis=1)
    return (sent_forward, sent_backward)
```

```python
import functools
import math

import jax
import jax.numpy as jnp
from jax import lax
from jax.experimental import pallas as pl
from jax.experimental.pallas import tpu as pltpu
from jax.sharding import PartitionSpec as P

QUERY_HEADS = 32
KEY_VALUE_HEADS = 4
HEAD_SIZE = 128

EPS = 1e-06
CHUNK = 512

VMEM = pl.BlockSpec(memory_space=pltpu.VMEM)
SMEM = pl.BlockSpec(memory_space=pltpu.SMEM)


def dot(former, latter):
    return jnp.dot(former, latter, preferred_element_type=jnp.float32)


def dot_back(former, latter):
    return lax.dot_general(
        former, latter, (((1,), (1,)), ((), ())), preferred_element_type=jnp.float32
    )


def dot_turned(former, latter):
    return lax.dot_general(
        former, latter, (((0,), (0,)), ((), ())), preferred_element_type=jnp.float32
    )


def rms_scale(matrix):
    return lax.rsqrt(jnp.mean(matrix * matrix, axis=-1, keepdims=True) + EPS)


def norm_back(upstream_in, grad_hat):
    scaling = rms_scale(upstream_in)
    return scaling * grad_hat - upstream_in * scaling**3 * jnp.mean(
        grad_hat * upstream_in, axis=-1, keepdims=True
    )


def spread(coeffs, expand_ref, gain_ref, query_ref, kv_ref, hidden_ref):
    width = expand_ref.shape[1]
    squares = jnp.zeros((coeffs.shape[0], 1), jnp.float32)
    for at in range(0, width, CHUNK):
        here = pl.ds(at, CHUNK)
        part = dot(coeffs, expand_ref[:, here])
        hidden_ref[:, here] = part
        squares += jnp.sum(part * part, axis=-1, keepdims=True)
    scaling = lax.rsqrt(squares / width + EPS)
    queries = jnp.zeros((coeffs.shape[0], query_ref.shape[1]), jnp.float32)
    kv = jnp.zeros((coeffs.shape[0], kv_ref.shape[1]), jnp.float32)
    for at in range(0, width, CHUNK):
        here = pl.ds(at, CHUNK)
        normed = (hidden_ref[:, here] * scaling * gain_ref[:, here]).astype(jnp.bfloat16)
        queries += dot(normed, query_ref[here, :])
        kv += dot(normed, kv_ref[here, :])
    return scaling, queries, kv[:, :HEAD_SIZE], kv[:, HEAD_SIZE:].astype(jnp.bfloat16)


def probabilities(q_hat, k_hat):
    rows = q_hat.shape[0]
    scores = dot_back(q_hat, k_hat) * (1.0 / math.sqrt(HEAD_SIZE))
    column = lax.broadcasted_iota(jnp.int32, (rows, rows), 1)
    row = lax.broadcasted_iota(jnp.int32, (rows, rows), 0)
    weights = jnp.where(column <= row, jnp.exp(scores), 0.0)
    return weights / jnp.sum(weights, axis=-1, keepdims=True)


def forward_kernel(
    coeffs_ref, expand_ref, gain_ref, query_ref, kv_ref, folded_ref, out_ref, hidden_ref
):
    scaling, queries, keys, values = spread(
        coeffs_ref[...], expand_ref, gain_ref, query_ref, kv_ref, hidden_ref
    )
    k_hat = (keys * rms_scale(keys)).astype(jnp.bfloat16)
    total = jnp.zeros(out_ref.shape, jnp.float32)
    for at in range(0, queries.shape[1], HEAD_SIZE):
        head = queries[:, at : at + HEAD_SIZE]
        q_hat = (head * rms_scale(head)).astype(jnp.bfloat16)
        low = probabilities(q_hat, k_hat).astype(jnp.bfloat16)
        attended = dot(low, values).astype(jnp.bfloat16)
        total += dot(attended, folded_ref[at : at + HEAD_SIZE, :])
    out_ref[...] = total.astype(out_ref.dtype)


def backward_kernel(
    flags_ref,
    stashed_ref,
    *refs,
):
    replays = refs[: flags_ref.shape[0]]
    (
        grads_ref,
        expand_ref,
        gain_ref,
        query_ref,
        kv_ref,
        folded_ref,
        out_ref,
        hidden_ref,
        weighted_ref,
    ) = refs[flags_ref.shape[0] :]
    coeffs = stashed_ref[...]
    for place, replay_ref in enumerate(replays):
        coeffs = jnp.where(flags_ref[place] != 0, replay_ref[...], coeffs)
    scaling, queries, keys, values = spread(
        coeffs, expand_ref, gain_ref, query_ref, kv_ref, hidden_ref
    )
    k_hat = (keys * rms_scale(keys)).astype(jnp.bfloat16)
    grads = grads_ref[...]
    grad_khat = jnp.zeros(keys.shape, jnp.float32)
    grad_values = jnp.zeros(keys.shape, jnp.float32)
    grad_queries = []
    for at in range(0, queries.shape[1], HEAD_SIZE):
        head = queries[:, at : at + HEAD_SIZE]
        q_hat = (head * rms_scale(head)).astype(jnp.bfloat16)
        weights = probabilities(q_hat, k_hat)
        grad_attended = dot_back(grads, folded_ref[at : at + HEAD_SIZE, :]).astype(jnp.bfloat16)
        grad_weights = dot_back(grad_attended, values)
        inner = jnp.sum(grad_weights * weights, axis=-1, keepdims=True)
        grad_scores = weights * (grad_weights - inner) * (1.0 / math.sqrt(HEAD_SIZE))
        grad_scores = grad_scores.astype(jnp.bfloat16)
        grad_qhat = dot(grad_scores, k_hat)
        grad_khat += dot_turned(grad_scores, q_hat)
        grad_values += dot_turned(weights.astype(jnp.bfloat16), grad_attended)
        grad_queries.append(norm_back(head, grad_qhat).astype(jnp.bfloat16))
    grad_queries = jnp.concatenate(grad_queries, axis=1)
    grad_kv = jnp.concatenate(
        [norm_back(keys, grad_khat).astype(jnp.bfloat16), grad_values.astype(jnp.bfloat16)], axis=1
    )
    width = expand_ref.shape[1]
    inner = jnp.zeros((coeffs.shape[0], 1), jnp.float32)
    for at in range(0, width, CHUNK):
        here = pl.ds(at, CHUNK)
        grad_normed = dot_back(grad_queries, query_ref[here, :]) + dot_back(grad_kv, kv_ref[here, :])
        weighted = grad_normed * gain_ref[:, here]
        weighted_ref[:, here] = weighted
        inner += jnp.sum(weighted * hidden_ref[:, here], axis=-1, keepdims=True)
    factor = scaling**3 * (inner / width)
    total = jnp.zeros(out_ref.shape, jnp.float32)
    for at in range(0, width, CHUNK):
        here = pl.ds(at, CHUNK)
        grad_hidden = scaling * weighted_ref[:, here] - hidden_ref[:, here] * factor
        total += dot_back(grad_hidden.astype(jnp.bfloat16), expand_ref[:, here])
    out_ref[...] = total.astype(out_ref.dtype)


def fold_kernel(expand_ref, compress_ref, out_weight_ref, basis_ref, folded_ref):
    basis_ref[...] = dot(expand_ref[...], compress_ref[...])
    folded_ref[...] = dot(out_weight_ref[...], compress_ref[...]).astype(folded_ref.dtype)


def finish_kernel(back, parts_ref, rows_ref, basis_ref, out_ref):
    direct = lax.dot_general(
        rows_ref[...].astype(jnp.float32),
        basis_ref[...],
        (((1,), (1 if back else 0,)), ((), ())),
        precision=lax.Precision.HIGHEST,
        preferred_element_type=jnp.float32,
    )
    summed = parts_ref[0].astype(jnp.float32)
    for place in range(1, parts_ref.shape[0]):
        summed += parts_ref[place].astype(jnp.float32)
    out_ref[...] = (summed + direct).astype(out_ref.dtype)


def in_vmem(body, outs, count, scratch=(), scalars=0, flops=0):
    return pl.pallas_call(
        body,
        out_shape=outs,
        in_specs=[SMEM] * scalars + [VMEM] * count,
        out_specs=jax.tree.map(lambda _: VMEM, outs),
        scratch_shapes=list(scratch),
        cost_estimate=pl.CostEstimate(flops=flops, bytes_accessed=2**20, transcendentals=0)
        if flops
        else None,
        compiler_params=pltpu.CompilerParams(vmem_limit_bytes=24 * 2**20),
    )


def shape_of(dims, kind):
    return jax.ShapeDtypeStruct(dims, kind)


def exchanged(x, axis):
    tiles = x.reshape(lax.axis_size(axis), -1, x.shape[-1])
    return lax.all_to_all(tiles, axis, split_axis=0, concat_axis=0, tiled=True)


def passed_along(x, axis, by):
    length = lax.axis_size(axis)
    pairs = [(i, i + by) for i in range(length) if 0 <= i + by < length]
    return lax.ppermute(x, axis, pairs)


def brought_to_first(x, axis):
    length = lax.axis_size(axis)
    step = 1
    while step < length:
        pairs = [(i, i - step) for i in range(step, length, 2 * step)]
        x = x + lax.ppermute(x, axis, pairs)
        step *= 2
    return x


def collect(x, axis):
    copies = jnp.broadcast_to(x, (lax.axis_size(axis), *x.shape))
    tiles = lax.all_to_all(copies, axis, split_axis=0, concat_axis=0, tiled=True)
    return tiles.reshape(-1, x.shape[-1])


def shards(
    token_ids,
    embed_table,
    arriving,
    returning,
    stashed,
    seed_grad,
    expand,
    compress,
    norm_gain,
    w_query,
    key_weight,
    value_weight,
    w_out,
):
    segment_index = lax.axis_index("segment")
    last_segment = lax.axis_size("segment") - 1
    head_index = lax.axis_index("head")
    is_first = segment_index == 0
    is_last = segment_index == last_segment
    ticks, span = token_ids.shape
    rank = embed_table.shape[1]
    share = span // lax.axis_size("head")
    start = head_index * share

    table_rows = embed_table.shape[0]
    first_row = lax.axis_index(("segment", "head")) * table_rows

    def picked(ids):
        local = ids - first_row
        inside = (local >= 0) & (local < table_rows)
        looked = jnp.take(embed_table, jnp.clip(local, 0, table_rows - 1), axis=0)
        return jnp.where(inside[:, None], looked, jnp.zeros((), looked.dtype))

    def own_rows_of(ids):
        return brought_to_first(exchanged(picked(ids), "head").sum(axis=0), "segment")

    embedded_rows = own_rows_of(token_ids[0])
    embedded = collect(embedded_rows, "head")
    later = exchanged(picked(token_ids[1:].reshape(-1)).reshape(ticks - 1, -1, share, rank).swapaxes(0, 1), "head")
    later = brought_to_first(later.reshape(-1, ticks - 1, share, rank).sum(axis=0), "segment")

    heads_here = w_query.shape[2] // HEAD_SIZE
    query_group_size = QUERY_HEADS // KEY_VALUE_HEADS
    first_kv = head_index * heads_here // query_group_size * HEAD_SIZE
    expand_here = expand[0]
    gain_here = norm_gain
    query_here = w_query[0]
    kv_here = jnp.concatenate(
        [
            lax.dynamic_slice_in_dim(key_weight[0], first_kv, HEAD_SIZE, 1),
            lax.dynamic_slice_in_dim(value_weight[0], first_kv, HEAD_SIZE, 1),
        ],
        axis=1,
    )
    width = expand_here.shape[1]
    low = jnp.bfloat16
    basis, folded = in_vmem(
        fold_kernel,
        (shape_of((rank, rank), jnp.float32), shape_of((w_out.shape[1], rank), low)),
        3,
    )(expand_here, compress[0], w_out[0])
    weights = (expand_here, gain_here, query_here, kv_here, folded)

    square = shape_of((span, rank), low)
    wide = pltpu.VMEM((span, width), jnp.float32)

    def forward(coeffs):
        return in_vmem(forward_kernel, square, 6, [wide])(coeffs, *weights)

    def backward(flags, stash, replays, grads):
        return in_vmem(backward_kernel, square, 7 + len(replays), [wide, wide], 1)(
            flags, stash, *replays, grads, *weights
        )

    def finish(partial, rows, back):
        return in_vmem(functools.partial(finish_kernel, back), shape_of((share, rank), low), 3)(
            exchanged(partial, "head"), rows, basis
        )

    def mine(x):
        return lax.dynamic_slice_in_dim(x, start, share, 0)

    forward_in = jnp.where(is_first, embedded, arriving[0])
    backward_in = jnp.where(is_last, seed_grad[0], returning[0])
    forward_rows = mine(forward_in)
    backward_rows = mine(backward_in)
    delay = 2 * (last_segment - segment_index)
    history = []
    apart = lax.axis_size("segment") > 2
    forward_shares = []
    backward_shares = []
    for tick in range(ticks):
        more = tick + 1 < ticks
        history.append(arriving[0] if tick == 0 and apart else forward_in)
        replays = [history[k] for k in range(tick + 1) if (tick - k) % 2 == 0]
        flags = jnp.stack(
            [(delay == tick - k).astype(jnp.int32) for k in range(tick + 1) if (tick - k) % 2 == 0]
        )
        out = finish(forward(forward_in), forward_rows, False)
        forward_shares.append(out)
        out_back = finish(
            backward(flags, stashed[0, tick], replays, backward_in), backward_rows, True
        )
        backward_shares.append(out_back)
        if more:
            arrived = passed_along(out, "segment", 1)
            forward_rows = jnp.where(is_first, later[tick], arrived)
            forward_in = collect(forward_rows, "head")
            arrived = passed_along(out_back, "segment", -1)
            backward_rows = jnp.where(is_last, mine(seed_grad[tick + 1]), arrived)
            backward_in = collect(backward_rows, "head")
    return (jnp.stack(forward_shares)[None], jnp.stack(backward_shares)[None])


def solution(mesh):
    return jax.shard_map(
        shards,
        mesh=mesh,
        in_specs=(
            P("groups", None),
            P(("segment", "head"), None),
            P(("groups", "segment"), None, None),
            P(("groups", "segment"), None, None),
            P(("groups", "segment"), None, None, None),
            P("groups", None, None),
            P("segment", None, None),
            P("segment", None, None),
            P("segment", None),
            P("segment", None, "head"),
            P("segment", None, None),
            P("segment", None, None),
            P("segment", "head", None),
        ),
        out_specs=(
            P(("groups", "segment"), None, "head", None),
            P(("groups", "segment"), None, "head", None),
        ),
        check_vma=False,
    )
```

```python
import functools
import math

import jax
import jax.numpy as jnp
from jax import lax
from jax.experimental import pallas as pl
from jax.experimental.pallas import tpu as pltpu
from jax.sharding import PartitionSpec as P

QUERY_HEADS = 32
KEY_VALUE_HEADS = 4
HEAD_SIZE = 128

EPS = 1e-06
CHUNK = 512
LANES = 128
LOW = jnp.bfloat16
WIDE = jnp.float32

VMEM = pl.BlockSpec(memory_space=pltpu.VMEM)
SMEM = pl.BlockSpec(memory_space=pltpu.SMEM)
HBM = pl.BlockSpec(memory_space=pltpu.HBM)


def dot(former, latter):
    return jnp.dot(former, latter, preferred_element_type=WIDE)


def dot_back(former, latter):
    return lax.dot_general(former, latter, (((1,), (1,)), ((), ())), preferred_element_type=WIDE)


def dot_turned(former, latter):
    return lax.dot_general(former, latter, (((0,), (0,)), ((), ())), preferred_element_type=WIDE)


def rms_scale(matrix):
    return lax.rsqrt(jnp.mean(matrix * matrix, axis=-1, keepdims=True) + EPS)


def norm_back(upstream_in, grad_hat):
    scaling = rms_scale(upstream_in)
    return scaling * grad_hat - upstream_in * scaling**3 * jnp.mean(
        grad_hat * upstream_in, axis=-1, keepdims=True
    )


def looped(count, body, carry, rolled):
    if rolled:
        return lax.fori_loop(0, count, body, carry)
    for place in range(count):
        carry = body(place, carry)
    return carry


def block(place, length):
    at = place * length
    return pl.ds(at if isinstance(at, int) else pl.multiple_of(at, length), length)


class Weights:
    def __init__(self, where_ref, hbm, vmem, sems):
        expand, query, key, value, folded = hbm
        self.expand, self.query, self.kv, self.folded = vmem
        first = pl.multiple_of(where_ref[1], HEAD_SIZE)
        self.count = self.expand.shape[0]
        copies = []
        for place in range(self.count):
            copies.append((expand.at[:, block(place, CHUNK)], self.expand.at[place]))
        copies.append((key.at[:, pl.ds(first, HEAD_SIZE)], self.kv.at[:, pl.ds(0, HEAD_SIZE)]))
        copies.append(
            (value.at[:, pl.ds(first, HEAD_SIZE)], self.kv.at[:, pl.ds(HEAD_SIZE, HEAD_SIZE)])
        )
        for place in range(self.count):
            copies.append((query.at[block(place, CHUNK), :], self.query.at[place]))
        copies.append((folded, self.folded))
        self.copies = [
            pltpu.make_async_copy(source, target, sems.at[place])
            for place, (source, target) in enumerate(copies)
        ]

    def start(self):
        for copy in self.copies:
            copy.start()

    def wait(self, first=0, last=None):
        for copy in self.copies[first:last]:
            copy.wait()


def weight_scratch(width, rank, queries):
    count = width // CHUNK
    return [
        pltpu.VMEM((count, rank, CHUNK), LOW),
        pltpu.VMEM((count, CHUNK, queries), LOW),
        pltpu.VMEM((width, 2 * HEAD_SIZE), LOW),
        pltpu.VMEM((queries, rank), LOW),
        pltpu.SemaphoreType.DMA((2 * count + 3,)),
    ]


STATE = 6


def state_shapes(span, width, queries):
    heads = queries // HEAD_SIZE
    return [
        ((width // CHUNK, span, CHUNK), WIDE),
        ((span, LANES), WIDE),
        ((heads, span, HEAD_SIZE), WIDE),
        ((span, HEAD_SIZE), WIDE),
        ((span, HEAD_SIZE), LOW),
        ((heads, span, span), WIDE),
    ]


def spread(coeffs, weights, gain_ref, state, rolled):
    hidden, scale, queries, keys, values, _ = state
    count = weights.count
    span = coeffs.shape[0]
    if rolled:
        weights.wait()

    def first(place, squares):
        if not rolled:
            weights.wait(place, place + 1)
        part = dot(coeffs, weights.expand[place])
        hidden[place] = part
        return squares + jnp.sum(part * part, axis=-1, keepdims=True)

    squares = looped(count, first, jnp.zeros((span, 1), WIDE), rolled)
    scaling = lax.rsqrt(squares / (count * CHUNK) + EPS)
    scale[...] = jnp.broadcast_to(scaling, scale.shape)
    if not rolled:
        weights.wait(count, count + 2)

    def second(place, carry):
        wide_q, wide_kv = carry
        if not rolled:
            weights.wait(count + 2 + place, count + 3 + place)
        normed = (hidden[place] * scaling * gain_ref[place]).astype(LOW)
        return (
            wide_q + dot(normed, weights.query[place]),
            wide_kv + dot(normed, weights.kv[block(place, CHUNK), :]),
        )

    heads = queries.shape[0]
    wide_q, wide_kv = looped(
        count,
        second,
        (
            jnp.zeros((span, heads * HEAD_SIZE), WIDE),
            jnp.zeros((span, 2 * HEAD_SIZE), WIDE),
        ),
        rolled,
    )
    for head in range(heads):
        queries[head] = wide_q[:, head * HEAD_SIZE : (head + 1) * HEAD_SIZE]
    keys[...] = wide_kv[:, :HEAD_SIZE]
    values[...] = wide_kv[:, HEAD_SIZE:].astype(LOW)


def hat(matrix):
    return (matrix * rms_scale(matrix)).astype(LOW)


def probabilities(q_hat, k_hat):
    rows = q_hat.shape[0]
    scores = dot_back(q_hat, k_hat) * (1.0 / math.sqrt(HEAD_SIZE))
    column = lax.broadcasted_iota(jnp.int32, (rows, rows), 1)
    row = lax.broadcasted_iota(jnp.int32, (rows, rows), 0)
    weights = jnp.where(column <= row, jnp.exp(scores), 0.0)
    return weights / jnp.sum(weights, axis=-1, keepdims=True)


def attend(weights, state, keep, rolled):
    _, _, queries, keys, values, probs = state
    k_hat = hat(keys[...])
    if not rolled:
        weights.wait(len(weights.copies) - 1)

    def one(head, total):
        chances = probabilities(hat(queries[head]), k_hat)
        if keep:
            probs[head] = chances
        if total is None:
            return None
        attended = dot(chances.astype(LOW), values[...]).astype(LOW)
        return total + dot(attended, weights.folded[block(head, HEAD_SIZE), :])

    span = keys.shape[0]
    start = jnp.zeros((span, weights.folded.shape[1]), WIDE)
    return looped(queries.shape[0], one, start, rolled)


def keep_probabilities(state, rolled):
    _, _, queries, keys, _, probs = state
    k_hat = hat(keys[...])

    def one(head, carry):
        probs[head] = probabilities(hat(queries[head]), k_hat)
        return carry

    looped(queries.shape[0], one, 0, rolled)


def go_back(grads, weights, gain_ref, state, grad_q, weighted_ref, rolled):
    hidden, scale, queries, keys, values, probs = state
    keys_here = keys[...]
    k_hat = hat(keys_here)
    values_here = values[...]

    def one(head, carry):
        grad_khat, grad_values = carry
        upstream = queries[head]
        q_hat = hat(upstream)
        chances = probs[head]
        grad_attended = dot_back(grads, weights.folded[block(head, HEAD_SIZE), :]).astype(LOW)
        grad_chances = dot_back(grad_attended, values_here)
        inner = jnp.sum(grad_chances * chances, axis=-1, keepdims=True)
        grad_scores = chances * (grad_chances - inner) * (1.0 / math.sqrt(HEAD_SIZE))
        grad_scores = grad_scores.astype(LOW)
        grad_q[:, block(head, HEAD_SIZE)] = norm_back(upstream, dot(grad_scores, k_hat)).astype(LOW)
        return (
            grad_khat + dot_turned(grad_scores, q_hat),
            grad_values + dot_turned(chances.astype(LOW), grad_attended),
        )

    empty = jnp.zeros(keys_here.shape, WIDE)
    grad_khat, grad_values = looped(queries.shape[0], one, (empty, empty), rolled)
    grad_kv = jnp.concatenate(
        [norm_back(keys_here, grad_khat).astype(LOW), grad_values.astype(LOW)], axis=1
    )
    scaling = scale[:, :1]

    def third(place, inner):
        grad_normed = dot_back(grad_q[...], weights.query[place]) + dot_back(
            grad_kv, weights.kv[block(place, CHUNK), :]
        )
        weighted = grad_normed * gain_ref[place]
        weighted_ref[place] = weighted
        return inner + jnp.sum(weighted * hidden[place], axis=-1, keepdims=True)

    inner = looped(weights.count, third, jnp.zeros((keys_here.shape[0], 1), WIDE), rolled)
    factor = scaling**3 * (inner / (weights.count * CHUNK))

    def fourth(place, total):
        grad_hidden = scaling * weighted_ref[place] - hidden[place] * factor
        return total + dot_back(grad_hidden.astype(LOW), weights.expand[place])

    return looped(weights.count, fourth, jnp.zeros(grads.shape, WIDE), rolled)


def direct_of(rows, basis_ref, back):
    return lax.dot_general(
        rows.astype(WIDE),
        basis_ref[...],
        (((1,), (1 if back else 0,)), ((), ())),
        precision=lax.Precision.HIGHEST,
        preferred_element_type=WIDE,
    )


def own_rows(ref, where_ref, share):
    return ref[pl.ds(pl.multiple_of(where_ref[0], share), share), :]


def put_tiles(payload_ref, total, at):
    share = payload_ref.shape[1] // 2
    for place in range(payload_ref.shape[0]):
        payload_ref[place, pl.ds(at, share), :] = total[place * share : (place + 1) * share].astype(
            LOW
        )


def state_kernel(where_ref, gain_ref, plain_ref, other_ref, *refs):
    hbm, outs, scratch = refs[:5], refs[5 : 5 + STATE], refs[5 + STATE :]
    weights = Weights(where_ref, hbm, scratch[:4], scratch[4])
    weights.start()
    coeffs = jnp.where(where_ref[2] != 0, other_ref[...], plain_ref[...])
    spread(coeffs, weights, gain_ref, outs, True)
    keep_probabilities(outs, True)


def first_back_kernel(where_ref, gain_ref, basis_ref, plain_ref, other_ref, grads_ref, *refs):
    hbm, outs, scratch = refs[:5], refs[5:7], refs[7:]
    weights = Weights(where_ref, hbm, scratch[:4], scratch[4])
    weights.start()
    grad_q, weighted, *state = scratch[5:]
    coeffs = jnp.where(where_ref[2] != 0, other_ref[...], plain_ref[...])
    spread(coeffs, weights, gain_ref, state, True)
    keep_probabilities(state, True)
    out_ref, direct_ref = outs
    total = go_back(grads_ref[...], weights, gain_ref, state, grad_q, weighted, True)
    out_ref[...] = total.astype(LOW)
    direct_ref[...] = direct_of(own_rows(grads_ref, where_ref, direct_ref.shape[0]), basis_ref, True)


def first_forward_kernel(where_ref, gain_ref, basis_ref, rows_ref, arriving_ref, back_ref, *refs):
    hbm, outs, scratch = refs[:5], refs[5:7], refs[7:]
    weights = Weights(where_ref, hbm, scratch[:4], scratch[4])
    weights.start()
    coeffs_ref, *state = scratch[5:]
    share = rows_ref.shape[1]
    for place in range(rows_ref.shape[0]):
        here = pl.ds(place * share, share)
        coeffs_ref[here, :] = jnp.where(where_ref[2] != 0, rows_ref[place], arriving_ref[here, :])
    payload_ref, direct_ref = outs
    direct_ref[...] = direct_of(own_rows(coeffs_ref, where_ref, share), basis_ref, False)
    spread(coeffs_ref[...], weights, gain_ref, [*state, None], False)
    put_tiles(payload_ref, attend(weights, [*state, None], False, False), 0)
    put_tiles(payload_ref, back_ref[...], share)


def both_kernel(where_ref, gain_ref, basis_ref, rows_ref, *refs):
    kept, hbm, outs, scratch = refs[:STATE], refs[STATE : STATE + 5], refs[STATE + 5 : STATE + 8], refs[STATE + 8 :]
    weights = Weights(where_ref, hbm, scratch[:4], scratch[4])
    weights.start()
    kept_sems, coeffs_ref, grads_ref, grad_q, weighted, *state = scratch[5:]
    copies = [
        pltpu.make_async_copy(source, target.at[1], kept_sems.at[place])
        for place, (source, target) in enumerate(zip(kept, state))
    ]
    for copy in copies:
        copy.start()
    payload_ref, direct_ref, direct_back_ref = outs
    share = rows_ref.shape[1] // 2
    for place in range(rows_ref.shape[0]):
        here = pl.ds(place * share, share)
        coeffs_ref[here, :] = rows_ref[place, pl.ds(0, share), :]
        grads_ref[here, :] = rows_ref[place, pl.ds(share, share), :]
    direct_ref[...] = direct_of(own_rows(coeffs_ref, where_ref, share), basis_ref, False)
    direct_back_ref[...] = direct_of(own_rows(grads_ref, where_ref, share), basis_ref, True)
    mine = [ref.at[0] for ref in state]
    spread(coeffs_ref[...], weights, gain_ref, mine, False)
    put_tiles(payload_ref, attend(weights, mine, True, False), 0)
    for copy in copies:
        copy.wait()
    slot = jnp.where(where_ref[3] != 0, 0, 1)
    chosen = [ref.at[slot] for ref in state]
    total = go_back(grads_ref[...], weights, gain_ref, chosen, grad_q, weighted, False)
    put_tiles(payload_ref, total, share)


def fold_kernel(expand_ref, compress_ref, out_weight_ref, basis_ref, folded_ref):
    basis_ref[...] = dot(expand_ref[...], compress_ref[...])
    folded_ref[...] = dot(out_weight_ref[...], compress_ref[...]).astype(folded_ref.dtype)


def finish_kernel(parts_ref, direct_ref, direct_back_ref, out_ref, out_back_ref):
    share = direct_ref.shape[0]
    for at, direct, out in ((0, direct_ref, out_ref), (share, direct_back_ref, out_back_ref)):
        summed = parts_ref[0, pl.ds(at, share), :].astype(WIDE)
        for place in range(1, parts_ref.shape[0]):
            summed += parts_ref[place, pl.ds(at, share), :].astype(WIDE)
        out[...] = (summed + direct[...]).astype(LOW)


def last_kernel(count, parts_ref, direct_ref, direct_back_ref, *refs):
    share = direct_ref.shape[0]
    before, out_ref, out_back_ref = refs[: 2 * count], refs[2 * count], refs[2 * count + 1]
    for place in range(count):
        out_ref[0, place] = before[place][...]
        out_back_ref[0, place] = before[count + place][...]
    finish_kernel(
        parts_ref, direct_ref, direct_back_ref, out_ref.at[0, count], out_back_ref.at[0, count]
    )


def mix_kernel(tick, where_ref, got_ref, got_back_ref, later_ref, seed_ref, out_ref):
    share = got_ref.shape[0]
    rows = jnp.where(where_ref[4] != 0, later_ref[pl.ds((tick + 1) * share, share), :], got_ref[...])
    seeds = own_rows(seed_ref.at[tick + 1], where_ref, share)
    rows_back = jnp.where(where_ref[5] != 0, seeds, got_back_ref[...])
    for place in range(out_ref.shape[0]):
        out_ref[place, pl.ds(0, share), :] = rows
        out_ref[place, pl.ds(share, share), :] = rows_back


def shape_of(dims, kind):
    return jax.ShapeDtypeStruct(dims, kind)


def call(body, outs, specs, scratch=(), flops=0):
    return pl.pallas_call(
        body,
        out_shape=outs,
        in_specs=specs,
        out_specs=jax.tree.map(lambda _: VMEM, outs),
        scratch_shapes=list(scratch),
        cost_estimate=pl.CostEstimate(flops=flops, bytes_accessed=2**20, transcendentals=0),
        compiler_params=pltpu.CompilerParams(vmem_limit_bytes=40 * 2**20),
    )


def exchanged(tiles, axis):
    return lax.all_to_all(tiles, axis, split_axis=0, concat_axis=0, tiled=True)


def passed_along(x, axis, by):
    length = lax.axis_size(axis)
    pairs = [(i, i + by) for i in range(length) if 0 <= i + by < length]
    return lax.ppermute(x, axis, pairs)


def brought_to_first(x, axis, radix):
    length = lax.axis_size(axis)
    step = 1
    while step < length:
        got = []
        for times in range(1, radix):
            pairs = [
                (i + times * step, i)
                for i in range(0, length, radix * step)
                if i + times * step < length
            ]
            if pairs:
                got.append(lax.ppermute(x, axis, pairs))
        for other in got:
            x = x + other
        step *= radix
    return x


def picked_rows(ids, first_row, table, parts, share):
    ticks = ids.shape[0]
    local = ids.reshape(ticks, parts, share).swapaxes(0, 1).reshape(-1) - first_row
    inside = (local >= 0) & (local < table.shape[0])
    looked = jnp.take(table, local, axis=0, mode="clip")
    looked = jnp.where(inside[:, None], looked, jnp.zeros((), looked.dtype))
    return looked.reshape(parts, ticks * share, -1)


def shards(
    token_ids,
    embed_table,
    arriving,
    returning,
    stashed,
    seed_grad,
    expand,
    compress,
    norm_gain,
    w_query,
    key_weight,
    value_weight,
    w_out,
):
    segment_index = lax.axis_index("segment")
    last_segment = lax.axis_size("segment") - 1
    head_index = lax.axis_index("head")
    parts = lax.axis_size("head")
    ticks, span = token_ids.shape
    rank = embed_table.shape[1]
    width = expand.shape[2]
    queries = w_query.shape[2]
    share = span // parts

    heads_here = queries // HEAD_SIZE
    query_group_size = QUERY_HEADS // KEY_VALUE_HEADS
    first_kv = head_index * heads_here // query_group_size * HEAD_SIZE
    delay = 2 * (last_segment - segment_index)

    def where(*flags):
        entries = [head_index * share, first_kv, *flags]
        return jnp.stack([jnp.asarray(entry, jnp.int32) for entry in entries])

    first_row = lax.axis_index(("segment", "head")) * embed_table.shape[0]
    tiles = exchanged(picked_rows(token_ids, first_row, embed_table, parts, share), "head")
    rows = brought_to_first(tiles.sum(axis=0), "segment", 4)
    embedded = exchanged(jnp.broadcast_to(rows[:share], (parts, share, rank)), "head")

    gain = norm_gain.reshape(-1, 1, CHUNK)
    square = shape_of((span, rank), LOW)
    payload = shape_of((parts, 2 * share, rank), LOW)
    piece = shape_of((share, rank), LOW)
    wide_piece = shape_of((share, rank), WIDE)
    basis, folded = call(
        fold_kernel,
        (shape_of((rank, rank), WIDE), shape_of((queries, rank), LOW)),
        [VMEM] * 3,
        flops=2 * (rank + queries) * width * rank,
    )(expand[0], compress[0], w_out[0])
    weights = (expand[0], w_query[0], key_weight[0], value_weight[0], folded)
    base = weight_scratch(width, rank, queries)
    states = state_shapes(span, width, queries)
    bits = pltpu.VMEM((span, queries), LOW)
    weighted = pltpu.VMEM((width // CHUNK, span, CHUNK), WIDE)
    lines = pltpu.VMEM((span, rank), LOW)
    work = 2 * span * width * (rank + queries + 2 * HEAD_SIZE)

    def kept_of(tick):
        return call(
            state_kernel,
            [shape_of(*entry) for entry in states],
            [SMEM] + [VMEM] * 3 + [HBM] * 5,
            base,
            flops=work,
        )(
            where(jnp.where((delay == tick) & (tick > 0), 1, 0)),
            gain,
            stashed[0, tick],
            arriving[0],
            *weights,
        )

    is_last = jnp.where(segment_index == last_segment, 1, 0)
    is_first = jnp.where(segment_index == 0, 1, 0)
    backward_in = jnp.where(is_last != 0, seed_grad[0], returning[0])
    back, direct_back = call(
        first_back_kernel,
        (square, wide_piece),
        [SMEM] + [VMEM] * 5 + [HBM] * 5,
        [*base, bits, weighted] + [pltpu.VMEM(*entry) for entry in states],
        flops=2 * work,
    )(where(is_last), gain, basis, stashed[0, 0], arriving[0], backward_in, *weights)
    kept = [kept_of(tick) for tick in range(1, ticks)]

    out, direct = call(
        first_forward_kernel,
        (payload, wide_piece),
        [SMEM] + [VMEM] * 5 + [HBM] * 5,
        [*base, lines] + [pltpu.VMEM(*entry) for entry in states[:-1]],
        flops=work,
    )(where(is_first), gain, basis, embedded, arriving[0], back, *weights)

    flags = where(0, is_last, is_first, is_last)
    shares = []
    for tick in range(ticks):
        arrived = exchanged(out, "head")
        if tick + 1 == ticks:
            break
        sent, sent_back = call(finish_kernel, (piece, piece), [VMEM] * 3)(
            arrived, direct, direct_back
        )
        shares.append((sent, sent_back))
        mixed = call(functools.partial(mix_kernel, tick), payload, [SMEM] + [VMEM] * 4)(
            flags,
            passed_along(sent, "segment", 1),
            passed_along(sent_back, "segment", -1),
            rows,
            seed_grad,
        )
        out, direct, direct_back = call(
            both_kernel,
            (payload, wide_piece, wide_piece),
            [SMEM] + [VMEM] * 3 + [HBM] * (STATE + 5),
            [*base, pltpu.SemaphoreType.DMA((STATE,)), lines, lines, bits, weighted]
            + [pltpu.VMEM((2, *dims), kind) for dims, kind in states],
            flops=2 * work,
        )(flags, gain, basis, exchanged(mixed, "head"), *kept[tick], *weights)
    whole = shape_of((1, ticks, share, rank), LOW)
    return call(functools.partial(last_kernel, ticks - 1), (whole, whole), [VMEM] * (3 + 2 * (ticks - 1)))(
        arrived, direct, direct_back, *[pair[0] for pair in shares], *[pair[1] for pair in shares]
    )


def solution(mesh):
    return jax.shard_map(
        shards,
        mesh=mesh,
        in_specs=(
            P("groups", None),
            P(("segment", "head"), None),
            P(("groups", "segment"), None, None),
            P(("groups", "segment"), None, None),
            P(("groups", "segment"), None, None, None),
            P("groups", None, None),
            P("segment", None, None),
            P("segment", None, None),
            P("segment", None),
            P("segment", None, "head"),
            P("segment", None, None),
            P("segment", None, None),
            P("segment", "head", None),
        ),
        out_specs=(
            P(("groups", "segment"), None, "head", None),
            P(("groups", "segment"), None, "head", None),
        ),
        check_vma=False,
    )
```

```python
import functools
import math

import jax
import jax.numpy as jnp
from jax import lax
from jax.experimental import pallas as pl
from jax.experimental.pallas import tpu as pltpu
from jax.sharding import PartitionSpec as P

QUERY_HEADS = 32
KEY_VALUE_HEADS = 4
HEAD_SIZE = 128

EPS = 1e-06
CHUNK = 512
LANES = 128
LOW = jnp.bfloat16
WIDE = jnp.float32

VMEM = pl.BlockSpec(memory_space=pltpu.VMEM)
SMEM = pl.BlockSpec(memory_space=pltpu.SMEM)
HBM = pl.BlockSpec(memory_space=pltpu.HBM)


def dot(former, latter):
    return jnp.dot(former, latter, preferred_element_type=WIDE)


def dot_back(former, latter):
    return lax.dot_general(former, latter, (((1,), (1,)), ((), ())), preferred_element_type=WIDE)


def dot_turned(former, latter):
    return lax.dot_general(former, latter, (((0,), (0,)), ((), ())), preferred_element_type=WIDE)


def rms_scale(matrix):
    return lax.rsqrt(jnp.mean(matrix * matrix, axis=-1, keepdims=True) + EPS)


def norm_back(upstream_in, grad_hat):
    scaling = rms_scale(upstream_in)
    return scaling * grad_hat - upstream_in * scaling**3 * jnp.mean(
        grad_hat * upstream_in, axis=-1, keepdims=True
    )


def block(place, length):
    at = place * length
    return pl.ds(at if isinstance(at, int) else pl.multiple_of(at, length), length)


STATE = 6


def state_shapes(span, width, queries):
    heads = queries // HEAD_SIZE
    return [
        ((width // CHUNK, span, CHUNK), WIDE),
        ((span, LANES), WIDE),
        ((heads, span, HEAD_SIZE), WIDE),
        ((span, HEAD_SIZE), WIDE),
        ((span, HEAD_SIZE), LOW),
        ((heads, span, span), WIDE),
    ]


def spread(coeffs, gain_ref, expand_ref, query_ref, kv_ref, state):
    hidden, scale, queries, keys, values, _ = state
    count = hidden.shape[0]
    span = coeffs.shape[0]
    squares = jnp.zeros((span, 1), WIDE)
    for place in range(count):
        part = dot(coeffs, expand_ref[:, block(place, CHUNK)])
        hidden[place] = part
        squares += jnp.sum(part * part, axis=-1, keepdims=True)
    scaling = lax.rsqrt(squares / (count * CHUNK) + EPS)
    scale[...] = jnp.broadcast_to(scaling, scale.shape)
    wide_q = jnp.zeros((span, query_ref.shape[1]), WIDE)
    wide_kv = jnp.zeros((span, kv_ref.shape[1]), WIDE)
    for place in range(count):
        normed = (hidden[place] * scaling * gain_ref[place]).astype(LOW)
        wide_q += dot(normed, query_ref[block(place, CHUNK), :])
        wide_kv += dot(normed, kv_ref[block(place, CHUNK), :])
    for head in range(queries.shape[0]):
        queries[head] = wide_q[:, head * HEAD_SIZE : (head + 1) * HEAD_SIZE]
    keys[...] = wide_kv[:, :HEAD_SIZE]
    values[...] = wide_kv[:, HEAD_SIZE:].astype(LOW)


def hat(matrix):
    return (matrix * rms_scale(matrix)).astype(LOW)


def probabilities(q_hat, k_hat):
    rows = q_hat.shape[0]
    scores = dot_back(q_hat, k_hat) * (1.0 / math.sqrt(HEAD_SIZE))
    column = lax.broadcasted_iota(jnp.int32, (rows, rows), 1)
    row = lax.broadcasted_iota(jnp.int32, (rows, rows), 0)
    weights = jnp.where(column <= row, jnp.exp(scores), 0.0)
    return weights / jnp.sum(weights, axis=-1, keepdims=True)


def attend(folded_ref, state):
    _, _, queries, keys, values, probs = state
    k_hat = hat(keys[...])
    total = None if folded_ref is None else jnp.zeros((keys.shape[0], folded_ref.shape[1]), WIDE)
    for head in range(queries.shape[0]):
        chances = probabilities(hat(queries[head]), k_hat)
        probs[head] = chances
        if folded_ref is not None:
            attended = dot(chances.astype(LOW), values[...]).astype(LOW)
            total += dot(attended, folded_ref[block(head, HEAD_SIZE), :])
    return total


def go_back(grads, gain_ref, expand_ref, query_ref, kv_ref, folded_ref, state, grad_q, weighted_ref):
    hidden, scale, queries, keys, values, probs = state
    count = hidden.shape[0]
    keys_here = keys[...]
    k_hat = hat(keys_here)
    values_here = values[...]
    grad_khat = jnp.zeros(keys_here.shape, WIDE)
    grad_values = jnp.zeros(keys_here.shape, WIDE)
    for head in range(queries.shape[0]):
        upstream = queries[head]
        q_hat = hat(upstream)
        chances = probs[head]
        grad_attended = dot_back(grads, folded_ref[block(head, HEAD_SIZE), :]).astype(LOW)
        grad_chances = dot_back(grad_attended, values_here)
        inner = jnp.sum(grad_chances * chances, axis=-1, keepdims=True)
        grad_scores = chances * (grad_chances - inner) * (1.0 / math.sqrt(HEAD_SIZE))
        grad_scores = grad_scores.astype(LOW)
        grad_q[:, block(head, HEAD_SIZE)] = norm_back(upstream, dot(grad_scores, k_hat)).astype(LOW)
        grad_khat += dot_turned(grad_scores, q_hat)
        grad_values += dot_turned(chances.astype(LOW), grad_attended)
    grad_kv = jnp.concatenate(
        [norm_back(keys_here, grad_khat).astype(LOW), grad_values.astype(LOW)], axis=1
    )
    scaling = scale[:, :1]
    inner = jnp.zeros((keys_here.shape[0], 1), WIDE)
    for place in range(count):
        grad_normed = dot_back(grad_q[...], query_ref[block(place, CHUNK), :]) + dot_back(
            grad_kv, kv_ref[block(place, CHUNK), :]
        )
        weighted = grad_normed * gain_ref[place]
        weighted_ref[place] = weighted
        inner += jnp.sum(weighted * hidden[place], axis=-1, keepdims=True)
    factor = scaling**3 * (inner / (count * CHUNK))
    total = jnp.zeros(grads.shape, WIDE)
    for place in range(count):
        grad_hidden = scaling * weighted_ref[place] - hidden[place] * factor
        total += dot_back(grad_hidden.astype(LOW), expand_ref[:, block(place, CHUNK)])
    return total


def direct_of(rows, basis_ref, back):
    return lax.dot_general(
        rows.astype(WIDE),
        basis_ref[...],
        (((1,), (1 if back else 0,)), ((), ())),
        precision=lax.Precision.HIGHEST,
        preferred_element_type=WIDE,
    )


def own_rows(ref, share):
    at = lax.axis_index("head") * share
    return ref[pl.ds(pl.multiple_of(at, share), share), :]


def place_in_line():
    return lax.axis_index("segment"), lax.axis_size("segment") - 1


def put_tiles(payload_ref, total, at):
    share = payload_ref.shape[1] // 2
    for place in range(payload_ref.shape[0]):
        payload_ref[place, pl.ds(at, share), :] = total[place * share : (place + 1) * share].astype(
            LOW
        )


def take_tiles(rows_ref, at, other_ref, use_other, out_ref):
    share = rows_ref.shape[1] // 2
    for place in range(rows_ref.shape[0]):
        here = pl.ds(place * share, share)
        out_ref[here, :] = jnp.where(
            use_other, other_ref[here, :], rows_ref[place, pl.ds(at, share), :]
        )


def state_kernel(
    tick_ref, gain_ref, order_ref, stash_ref, other_ref, expand_ref, query_ref, kv_ref, *refs
):
    state, token_ref = [ref.at[1] for ref in refs[:STATE]], refs[STATE]
    segment, last = place_in_line()
    use_other = 2 * (last - segment) == tick_ref[0]
    coeffs = jnp.where(use_other, other_ref[...], stash_ref[...])
    spread(coeffs, gain_ref, expand_ref, query_ref, kv_ref, state)
    attend(None, state)
    token_ref[...] = jnp.zeros(token_ref.shape, LOW)


def forward_kernel(
    tick_ref, gain_ref, basis_ref, rows_ref, other_ref, expand_ref, query_ref, kv_ref, folded_ref, *refs
):
    payload_ref, direct_ref, coeffs_ref = refs[1 + STATE], refs[2 + 2 * STATE], refs[3 + 2 * STATE]
    state = [ref.at[0] for ref in refs[2 + STATE : 2 + 2 * STATE]]
    segment, _ = place_in_line()
    use_other = (tick_ref[0] == 0) & (segment != 0)
    take_tiles(rows_ref, 0, other_ref, use_other, coeffs_ref)
    direct_ref[...] = direct_of(own_rows(coeffs_ref, direct_ref.shape[0]), basis_ref, False)
    spread(coeffs_ref[...], gain_ref, expand_ref, query_ref, kv_ref, state)
    put_tiles(payload_ref, attend(folded_ref, state), 0)


def backward_kernel(
    tick_ref, gain_ref, basis_ref, rows_ref, other_ref, expand_ref, query_ref, kv_ref, folded_ref, *refs
):
    kept = refs[1 : 1 + STATE]
    payload_ref, direct_ref, token_ref, grads_ref, grad_q, weighted = refs[1 + STATE :]
    share = direct_ref.shape[0]
    segment, last = place_in_line()
    take_tiles(rows_ref, share, other_ref, tick_ref[0] == 0, grads_ref)
    direct_ref[...] = direct_of(own_rows(grads_ref, share), basis_ref, True)
    slot = jnp.where((tick_ref[0] != 0) & (segment == last), 0, 1)
    state = [ref.at[slot] for ref in kept]
    total = go_back(
        grads_ref[...], gain_ref, expand_ref, query_ref, kv_ref, folded_ref, state, grad_q, weighted
    )
    put_tiles(payload_ref, total, share)
    token_ref[...] = jnp.zeros(token_ref.shape, LOW)


def fold_kernel(expand_ref, compress_ref, out_weight_ref, key_ref, value_ref, basis_ref, folded_ref, kv_ref, sems):
    heads_here = out_weight_ref.shape[0] // HEAD_SIZE
    first = lax.axis_index("head") * heads_here * KEY_VALUE_HEADS // QUERY_HEADS * HEAD_SIZE
    here = pl.ds(pl.multiple_of(first, HEAD_SIZE), HEAD_SIZE)
    copies = [
        pltpu.make_async_copy(
            ref.at[:, here], kv_ref.at[:, pl.ds(place * HEAD_SIZE, HEAD_SIZE)], sems.at[place]
        )
        for place, ref in enumerate((key_ref, value_ref))
    ]
    for copy in copies:
        copy.start()
    basis_ref[...] = dot(expand_ref[...], compress_ref[...])
    folded_ref[...] = dot(out_weight_ref[...], compress_ref[...]).astype(folded_ref.dtype)
    for copy in copies:
        copy.wait()


def finish_kernel(parts_ref, direct_ref, direct_back_ref, out_ref, out_back_ref):
    share = direct_ref.shape[0]
    for at, direct, out in ((0, direct_ref, out_ref), (share, direct_back_ref, out_back_ref)):
        summed = parts_ref[0, pl.ds(at, share), :].astype(WIDE)
        for place in range(1, parts_ref.shape[0]):
            summed += parts_ref[place, pl.ds(at, share), :].astype(WIDE)
        out[...] = (summed + direct[...]).astype(LOW)


def last_kernel(count, parts_ref, direct_ref, direct_back_ref, *refs):
    share = direct_ref.shape[0]
    before, out_ref, out_back_ref = refs[: 2 * count], refs[2 * count], refs[2 * count + 1]
    for place in range(count):
        out_ref[0, place] = before[place][...]
        out_back_ref[0, place] = before[count + place][...]
    finish_kernel(
        parts_ref, direct_ref, direct_back_ref, out_ref.at[0, count], out_back_ref.at[0, count]
    )


def mix_kernel(tick_ref, got_ref, got_back_ref, later_ref, seed_ref, out_ref):
    share = got_ref.shape[0]
    tick = tick_ref[0]
    segment, last = place_in_line()
    later = later_ref[pl.ds(pl.multiple_of(tick * share, share), share), :]
    rows = jnp.where(segment == 0, later, got_ref[...])
    rows_back = jnp.where(segment == last, own_rows(seed_ref.at[tick], share), got_back_ref[...])
    for place in range(out_ref.shape[0]):
        out_ref[place, pl.ds(0, share), :] = rows
        out_ref[place, pl.ds(share, share), :] = rows_back


def shape_of(dims, kind):
    return jax.ShapeDtypeStruct(dims, kind)


def call(body, outs, specs, scratch=(), flops=0, aliases=None, limit=8):
    kernel = pl.pallas_call(
        body,
        out_shape=outs,
        in_specs=specs,
        out_specs=jax.tree.map(lambda _: VMEM, outs),
        scratch_shapes=list(scratch),
        input_output_aliases=aliases or {},
        cost_estimate=pl.CostEstimate(flops=flops, bytes_accessed=2**20, transcendentals=0),
        compiler_params=pltpu.CompilerParams(vmem_limit_bytes=limit * 2**20),
    )

    def run(*args):
        return kernel(
            *[
                pltpu.with_memory_space_constraint(arg, pltpu.HBM) if spec is HBM else arg
                for spec, arg in zip(specs, args)
            ]
        )

    return run


def exchanged(tiles, axis):
    return lax.all_to_all(tiles, axis, split_axis=0, concat_axis=0, tiled=True)


def passed_along(x, axis, by):
    length = lax.axis_size(axis)
    pairs = [(i, i + by) for i in range(length) if 0 <= i + by < length]
    return lax.ppermute(x, axis, pairs)


def brought_to_first(x, axis, radix, fillers):
    length = lax.axis_size(axis)
    step = 1
    while step < length:
        got = []
        for times in range(1, radix):
            pairs = [
                (i + times * step, i)
                for i in range(0, length, radix * step)
                if i + times * step < length
            ]
            if pairs:
                got.append(lax.ppermute(x, axis, pairs))
        beside = fillers.pop(0)(x) if fillers else None
        for other in got:
            x = x + other
        if beside is not None:
            x = x + beside[0, 0]
        step *= radix
    for filler in fillers:
        x = x + filler(x)[0, 0]
    return x


def picked_rows(ids, first_row, table, parts, share):
    ticks = ids.shape[0]
    local = ids.reshape(ticks, parts, share).swapaxes(0, 1).reshape(-1) - first_row
    inside = (local >= 0) & (local < table.shape[0])
    looked = jnp.take(table, local, axis=0, mode="clip")
    looked = jnp.where(inside[:, None], looked, jnp.zeros((), looked.dtype))
    return looked.reshape(parts, ticks * share, -1)


def shards(
    token_ids,
    embed_table,
    arriving,
    returning,
    stashed,
    seed_grad,
    expand,
    compress,
    norm_gain,
    w_query,
    key_weight,
    value_weight,
    w_out,
):
    segment_index = lax.axis_index("segment")
    last_segment = lax.axis_size("segment") - 1
    head_index = lax.axis_index("head")
    parts = lax.axis_size("head")
    ticks, span = token_ids.shape
    rank = embed_table.shape[1]
    width = expand.shape[2]
    queries = w_query.shape[2]
    share = span // parts

    def number(tick):
        return jnp.full((1,), tick, jnp.int32)

    first_row = lax.axis_index(("segment", "head")) * embed_table.shape[0]
    tiles = exchanged(picked_rows(token_ids, first_row, embed_table, parts, share), "head")

    gain = norm_gain.reshape(-1, 1, CHUNK)
    payload = shape_of((parts, 2 * share, rank), LOW)
    piece = shape_of((share, rank), LOW)
    wide_piece = shape_of((share, rank), WIDE)
    token = shape_of((16, 128), LOW)
    basis, folded, kv = call(
        fold_kernel,
        (
            shape_of((rank, rank), WIDE),
            shape_of((queries, rank), LOW),
            shape_of((width, 2 * HEAD_SIZE), LOW),
        ),
        [VMEM] * 3 + [HBM] * 2,
        [pltpu.SemaphoreType.DMA((2,))],
        flops=2 * (rank + queries) * width * rank,
    )(expand[0], compress[0], w_out[0], key_weight[0], value_weight[0])
    weights = (expand[0], w_query[0], kv, folded)
    states = [((2, *dims), kind) for dims, kind in state_shapes(span, width, queries)]
    state_outs = tuple(shape_of(*entry) for entry in states)
    work = 2 * span * width * (rank + queries + 2 * HEAD_SIZE)
    lines = pltpu.VMEM((span, rank), LOW)

    def kept_of(tick, order):
        *state, done = call(
            state_kernel,
            (*state_outs, token),
            [SMEM] + [VMEM] * 7,
            flops=work,
        )(number(tick), gain, order, stashed[0, tick], arriving[0], *weights[:3])
        return state, done

    def forward(tick, rows, other, out, state):
        out, *state, direct = call(
            forward_kernel,
            (payload, *state_outs, wide_piece),
            [SMEM] + [VMEM] * (9 + STATE),
            [lines],
            flops=work,
            aliases={9 + place: place for place in range(1 + STATE)},
        )(number(tick), gain, basis, rows, other, *weights, out, *state)
        return out, state, direct

    def backward(tick, rows, other, out, state):
        return call(
            backward_kernel,
            (payload, wide_piece, token),
            [SMEM] + [VMEM] * (9 + STATE),
            [lines, pltpu.VMEM((span, queries), LOW), pltpu.VMEM((width // CHUNK, span, CHUNK), WIDE)],
            flops=work,
            aliases={9: 0},
        )(number(tick), gain, basis, rows, other, *weights, out, *state)

    segment_index = lax.axis_index("segment")
    is_last = segment_index == lax.axis_size("segment") - 1
    backward_in = jnp.where(is_last, seed_grad[0], returning[0])
    state, _ = kept_of(0, jnp.zeros((ticks * share, rank), LOW))
    empty = jnp.zeros(payload.shape, LOW)
    out, direct_back, done = backward(0, empty, backward_in, empty, state)

    kept = []

    def filler(tick, order):
        state, done = kept_of(tick, order)
        kept.append(state)
        return done

    rows = brought_to_first(
        tiles.sum(axis=0) + done[0, 0],
        "segment",
        4,
        [functools.partial(filler, tick) for tick in range(1, ticks)],
    )
    gathered = exchanged(jnp.broadcast_to(rows[: 2 * share], payload.shape), "head")

    shares = []
    out, kept[0], direct = forward(0, gathered, arriving[0], out, kept[0])
    for tick in range(1, ticks):
        sent, sent_back = call(finish_kernel, (piece, piece), [VMEM] * 3, limit=4)(
            exchanged(out, "head"), direct, direct_back
        )
        shares.append((sent, sent_back))
        mixed = call(mix_kernel, payload, [SMEM] + [VMEM] * 4, limit=4)(
            number(tick),
            passed_along(sent, "segment", 1),
            passed_along(sent_back, "segment", -1),
            rows,
            seed_grad,
        )
        gathered = exchanged(mixed, "head")
        out, state, direct = forward(tick, gathered, arriving[0], out, kept[tick - 1])
        out, direct_back, _ = backward(tick, gathered, arriving[0], out, state)
    whole = shape_of((1, ticks, share, rank), LOW)
    return call(
        functools.partial(last_kernel, ticks - 1),
        (whole, whole),
        [VMEM] * (3 + 2 * (ticks - 1)),
        limit=4,
    )(
        exchanged(out, "head"),
        direct,
        direct_back,
        *[pair[0] for pair in shares],
        *[pair[1] for pair in shares],
    )


def solution(mesh):
    return jax.shard_map(
        shards,
        mesh=mesh,
        in_specs=(
            P("groups", None),
            P(("segment", "head"), None),
            P(("groups", "segment"), None, None),
            P(("groups", "segment"), None, None),
            P(("groups", "segment"), None, None, None),
            P("groups", None, None),
            P("segment", None, None),
            P("segment", None, None),
            P("segment", None),
            P("segment", None, "head"),
            P("segment", None, None),
            P("segment", None, None),
            P("segment", "head", None),
        ),
        out_specs=(
            P(("groups", "segment"), None, "head", None),
            P(("groups", "segment"), None, "head", None),
        ),
        check_vma=False,
    )
```

```python
import functools
import math

import jax
import jax.numpy as jnp
from jax import lax
from jax.experimental import pallas as pl
from jax.experimental.pallas import tpu as pltpu
from jax.sharding import PartitionSpec as P

QUERY_HEADS = 32
KEY_VALUE_HEADS = 4
HEAD_SIZE = 128

EPS = 1e-06
CHUNK = 512
LANES = 128
RADIX = 4
LOW = jnp.bfloat16
WIDE = jnp.float32

VMEM = pl.BlockSpec(memory_space=pltpu.VMEM)
SMEM = pl.BlockSpec(memory_space=pltpu.SMEM)
HBM = pl.BlockSpec(memory_space=pltpu.HBM)


def dot(former, latter):
    return jnp.dot(former, latter, preferred_element_type=WIDE)


def dot_back(former, latter):
    return lax.dot_general(former, latter, (((1,), (1,)), ((), ())), preferred_element_type=WIDE)


def dot_turned(former, latter):
    return lax.dot_general(former, latter, (((0,), (0,)), ((), ())), preferred_element_type=WIDE)


def rms_scale(matrix):
    return lax.rsqrt(jnp.mean(matrix * matrix, axis=-1, keepdims=True) + EPS)


def norm_back(upstream_in, grad_hat):
    scaling = rms_scale(upstream_in)
    return scaling * grad_hat - upstream_in * scaling**3 * jnp.mean(
        grad_hat * upstream_in, axis=-1, keepdims=True
    )


def block(place, length):
    at = place * length
    return pl.ds(at if isinstance(at, int) else pl.multiple_of(at, length), length)


STATE = 6


def state_shapes(span, width, queries):
    heads = queries // HEAD_SIZE
    return [
        ((width // CHUNK, span, CHUNK), WIDE),
        ((span, LANES), WIDE),
        ((heads, span, HEAD_SIZE), WIDE),
        ((span, HEAD_SIZE), WIDE),
        ((span, HEAD_SIZE), LOW),
        ((heads, span, span), WIDE),
    ]


def spread(coeffs, gain_ref, expand_ref, query_ref, kv_ref, state):
    hidden, scale, queries, keys, values, _ = state
    count = hidden.shape[0]
    span = coeffs.shape[0]
    squares = jnp.zeros((span, 1), WIDE)
    for place in range(count):
        part = dot(coeffs, expand_ref[:, block(place, CHUNK)])
        hidden[place] = part
        squares += jnp.sum(part * part, axis=-1, keepdims=True)
    scaling = lax.rsqrt(squares / (count * CHUNK) + EPS)
    scale[...] = jnp.broadcast_to(scaling, scale.shape)
    wide_q = jnp.zeros((span, query_ref.shape[1]), WIDE)
    wide_kv = jnp.zeros((span, kv_ref.shape[1]), WIDE)
    for place in range(count):
        normed = (hidden[place] * scaling * gain_ref[place]).astype(LOW)
        wide_q += dot(normed, query_ref[block(place, CHUNK), :])
        wide_kv += dot(normed, kv_ref[block(place, CHUNK), :])
    for head in range(queries.shape[0]):
        queries[head] = wide_q[:, head * HEAD_SIZE : (head + 1) * HEAD_SIZE]
    keys[...] = wide_kv[:, :HEAD_SIZE]
    values[...] = wide_kv[:, HEAD_SIZE:].astype(LOW)


def hat(matrix):
    return (matrix * rms_scale(matrix)).astype(LOW)


def probabilities(q_hat, k_hat):
    rows = q_hat.shape[0]
    scores = dot_back(q_hat, k_hat) * (1.0 / math.sqrt(HEAD_SIZE))
    column = lax.broadcasted_iota(jnp.int32, (rows, rows), 1)
    row = lax.broadcasted_iota(jnp.int32, (rows, rows), 0)
    weights = jnp.where(column <= row, jnp.exp(scores), 0.0)
    return weights / jnp.sum(weights, axis=-1, keepdims=True)


def attend(folded_ref, state):
    _, _, queries, keys, values, probs = state
    k_hat = hat(keys[...])
    total = None if folded_ref is None else jnp.zeros((keys.shape[0], folded_ref.shape[1]), WIDE)
    for head in range(queries.shape[0]):
        chances = probabilities(hat(queries[head]), k_hat)
        probs[head] = chances
        if folded_ref is not None:
            attended = dot(chances.astype(LOW), values[...]).astype(LOW)
            total += dot(attended, folded_ref[block(head, HEAD_SIZE), :])
    return total


def go_back(grads, gain_ref, expand_ref, query_ref, kv_ref, folded_ref, state, grad_q, weighted_ref):
    hidden, scale, queries, keys, values, probs = state
    count = hidden.shape[0]
    keys_here = keys[...]
    k_hat = hat(keys_here)
    values_here = values[...]
    grad_khat = jnp.zeros(keys_here.shape, WIDE)
    grad_values = jnp.zeros(keys_here.shape, WIDE)
    for head in range(queries.shape[0]):
        upstream = queries[head]
        q_hat = hat(upstream)
        chances = probs[head]
        grad_attended = dot_back(grads, folded_ref[block(head, HEAD_SIZE), :]).astype(LOW)
        grad_chances = dot_back(grad_attended, values_here)
        inner = jnp.sum(grad_chances * chances, axis=-1, keepdims=True)
        grad_scores = chances * (grad_chances - inner) * (1.0 / math.sqrt(HEAD_SIZE))
        grad_scores = grad_scores.astype(LOW)
        grad_q[:, block(head, HEAD_SIZE)] = norm_back(upstream, dot(grad_scores, k_hat)).astype(LOW)
        grad_khat += dot_turned(grad_scores, q_hat)
        grad_values += dot_turned(chances.astype(LOW), grad_attended)
    grad_kv = jnp.concatenate(
        [norm_back(keys_here, grad_khat).astype(LOW), grad_values.astype(LOW)], axis=1
    )
    scaling = scale[:, :1]
    inner = jnp.zeros((keys_here.shape[0], 1), WIDE)
    for place in range(count):
        grad_normed = dot_back(grad_q[...], query_ref[block(place, CHUNK), :]) + dot_back(
            grad_kv, kv_ref[block(place, CHUNK), :]
        )
        weighted = grad_normed * gain_ref[place]
        weighted_ref[place] = weighted
        inner += jnp.sum(weighted * hidden[place], axis=-1, keepdims=True)
    factor = scaling**3 * (inner / (count * CHUNK))
    total = jnp.zeros(grads.shape, WIDE)
    for place in range(count):
        grad_hidden = scaling * weighted_ref[place] - hidden[place] * factor
        total += dot_back(grad_hidden.astype(LOW), expand_ref[:, block(place, CHUNK)])
    return total


def direct_of(rows, basis_ref, back):
    return lax.dot_general(
        rows.astype(WIDE),
        basis_ref[...],
        (((1,), (1 if back else 0,)), ((), ())),
        precision=lax.Precision.HIGHEST,
        preferred_element_type=WIDE,
    )


def own_rows(ref, share):
    at = lax.axis_index("head") * share
    return ref[pl.ds(pl.multiple_of(at, share), share), :]


def place_in_line():
    return lax.axis_index("segment"), lax.axis_size("segment") - 1


def put_tiles(payload_ref, total, at):
    share = payload_ref.shape[1] // 2
    for place in range(payload_ref.shape[0]):
        payload_ref[place, pl.ds(at, share), :] = total[place * share : (place + 1) * share].astype(
            LOW
        )


def take_tiles(rows_ref, at, other_ref, use_other, out_ref):
    share = rows_ref.shape[1] // 2
    for place in range(rows_ref.shape[0]):
        here = pl.ds(place * share, share)
        out_ref[here, :] = jnp.where(
            use_other, other_ref[here, :], rows_ref[place, pl.ds(at, share), :]
        )


def state_kernel(
    tick_ref, gain_ref, order_ref, stash_ref, other_ref, expand_ref, query_ref, kv_ref, *refs
):
    state = [ref.at[1] for ref in refs[:STATE]]
    segment, last = place_in_line()
    use_other = 2 * (last - segment) == tick_ref[0]
    coeffs = jnp.where(use_other, other_ref[...], stash_ref[tick_ref[0]])
    spread(coeffs, gain_ref, expand_ref, query_ref, kv_ref, state)
    attend(None, state)
    refs[STATE][...] = jnp.zeros(refs[STATE].shape, LOW)


def forward_kernel(
    tick_ref, gain_ref, basis_ref, rows_ref, other_ref, expand_ref, query_ref, kv_ref, folded_ref, *refs
):
    payload_ref, direct_ref, coeffs_ref = refs[1 + STATE], refs[2 + 2 * STATE], refs[3 + 2 * STATE]
    state = [ref.at[0] for ref in refs[2 + STATE : 2 + 2 * STATE]]
    segment, _ = place_in_line()
    use_other = (tick_ref[0] == 0) & (segment != 0)
    take_tiles(rows_ref, 0, other_ref, use_other, coeffs_ref)
    direct_ref[...] = direct_of(own_rows(coeffs_ref, direct_ref.shape[0]), basis_ref, False)
    spread(coeffs_ref[...], gain_ref, expand_ref, query_ref, kv_ref, state)
    put_tiles(payload_ref, attend(folded_ref, state), 0)


def backward_kernel(
    tick_ref,
    gain_ref,
    basis_ref,
    rows_ref,
    returning_ref,
    seed_ref,
    expand_ref,
    query_ref,
    kv_ref,
    folded_ref,
    *refs,
):
    kept = refs[1 : 1 + STATE]
    payload_ref, direct_ref, token_ref, grads_ref, grad_q, weighted = refs[1 + STATE :]
    share = direct_ref.shape[0]
    segment, last = place_in_line()
    first_tick = tick_ref[0] == 0
    for place in range(rows_ref.shape[0]):
        here = pl.ds(place * share, share)
        given = jnp.where(segment == last, seed_ref[0, here, :], returning_ref[here, :])
        grads_ref[here, :] = jnp.where(first_tick, given, rows_ref[place, pl.ds(share, share), :])
    direct_ref[...] = direct_of(own_rows(grads_ref, share), basis_ref, True)
    slot = jnp.where(jnp.logical_not(first_tick) & (segment == last), 0, 1)
    state = [ref.at[slot] for ref in kept]
    total = go_back(
        grads_ref[...], gain_ref, expand_ref, query_ref, kv_ref, folded_ref, state, grad_q, weighted
    )
    put_tiles(payload_ref, total, share)
    token_ref[...] = jnp.zeros(token_ref.shape, LOW)


def pick_kernel(ids_ref, table_ref, out_ref):
    rows = table_ref.shape[0]
    full = rows // LANES * LANES
    ticks, span = ids_ref.shape
    share = out_ref.shape[1] // ticks
    own = lax.axis_index("segment") * lax.axis_size("head") + lax.axis_index("head")
    lane = lax.broadcasted_iota(jnp.int32, (LANES, LANES), 1).astype(WIDE)

    def chosen(names, at):
        return jnp.where(names == lane + float(at), 1.0, 0.0).astype(LOW)

    for tick in range(ticks):
        for at in range(0, span, LANES):
            local = (ids_ref[tick : tick + 1, at : at + LANES] - own * rows).astype(WIDE)
            names = jnp.broadcast_to(local, (LANES, LANES)).T
            hits = jnp.concatenate([chosen(names, k) for k in range(0, full, LANES)], axis=1)
            found = dot(hits, table_ref[pl.ds(0, full), :])
            if rows > full:
                found += dot(
                    chosen(names, full)[:, : rows - full], table_ref[pl.ds(full, rows - full), :]
                )
            for place in range(LANES // share):
                out_ref[at // share + place, pl.ds(tick * share, share), :] = found[
                    place * share : (place + 1) * share
                ].astype(LOW)


def sum_kernel(parts_ref, out_ref, order_ref):
    total = parts_ref[0]
    for place in range(1, parts_ref.shape[0]):
        total += parts_ref[place]
    out_ref[...] = total
    order_ref[...] = total[: order_ref.shape[0]]


def join_kernel(count, rows_ref, *refs):
    got, (token_ref, out_ref, *tiles) = refs[:count], refs[count:]
    total = rows_ref[...]
    for ref in got:
        total += ref[...]
    out_ref[...] = total
    for ref in tiles:
        for place in range(ref.shape[0]):
            ref[place] = total[: ref.shape[1]]


def fold_kernel(
    order_ref, expand_ref, compress_ref, out_weight_ref, key_ref, value_ref, basis_ref, folded_ref, kv_ref, sems
):
    heads_here = out_weight_ref.shape[0] // HEAD_SIZE
    first = lax.axis_index("head") * heads_here * KEY_VALUE_HEADS // QUERY_HEADS * HEAD_SIZE
    here = pl.ds(pl.multiple_of(first, HEAD_SIZE), HEAD_SIZE)
    copies = [
        pltpu.make_async_copy(
            ref.at[:, here], kv_ref.at[:, pl.ds(place * HEAD_SIZE, HEAD_SIZE)], sems.at[place]
        )
        for place, ref in enumerate((key_ref, value_ref))
    ]
    for copy in copies:
        copy.start()
    basis_ref[...] = dot(expand_ref[...], compress_ref[...])
    folded_ref[...] = dot(out_weight_ref[...], compress_ref[...]).astype(folded_ref.dtype)
    for copy in copies:
        copy.wait()


def finish_kernel(parts_ref, direct_ref, direct_back_ref, out_ref, out_back_ref):
    share = direct_ref.shape[0]
    for at, direct, out in ((0, direct_ref, out_ref), (share, direct_back_ref, out_back_ref)):
        summed = parts_ref[0, pl.ds(at, share), :].astype(WIDE)
        for place in range(1, parts_ref.shape[0]):
            summed += parts_ref[place, pl.ds(at, share), :].astype(WIDE)
        out[...] = (summed + direct[...]).astype(LOW)


def last_kernel(count, parts_ref, direct_ref, direct_back_ref, *refs):
    share = direct_ref.shape[0]
    before, out_ref, out_back_ref = refs[: 2 * count], refs[2 * count], refs[2 * count + 1]
    for place in range(count):
        out_ref[0, place] = before[place][...]
        out_back_ref[0, place] = before[count + place][...]
    finish_kernel(
        parts_ref, direct_ref, direct_back_ref, out_ref.at[0, count], out_back_ref.at[0, count]
    )


def mix_kernel(tick_ref, got_ref, got_back_ref, later_ref, seed_ref, token_ref, out_ref):
    share = got_ref.shape[0]
    tick = tick_ref[0]
    segment, last = place_in_line()
    later = later_ref[pl.ds(pl.multiple_of(tick * share, share), share), :]
    rows = jnp.where(segment == 0, later, got_ref[...])
    rows_back = jnp.where(segment == last, own_rows(seed_ref.at[tick], share), got_back_ref[...])
    for place in range(out_ref.shape[0]):
        out_ref[place, pl.ds(0, share), :] = rows
        out_ref[place, pl.ds(share, share), :] = rows_back


def shape_of(dims, kind):
    return jax.ShapeDtypeStruct(dims, kind)


def call(body, outs, specs, scratch=(), flops=0, aliases=None, limit=8):
    kernel = pl.pallas_call(
        body,
        out_shape=outs,
        in_specs=specs,
        out_specs=jax.tree.map(lambda _: VMEM, outs),
        scratch_shapes=list(scratch),
        input_output_aliases=aliases or {},
        cost_estimate=pl.CostEstimate(flops=flops, bytes_accessed=2**20, transcendentals=0),
        compiler_params=pltpu.CompilerParams(vmem_limit_bytes=limit * 2**20),
    )

    def run(*args):
        return kernel(
            *[
                pltpu.with_memory_space_constraint(arg, pltpu.HBM) if spec is HBM else arg
                for spec, arg in zip(specs, args)
            ]
        )

    return run


def exchanged(tiles, axis):
    return lax.all_to_all(tiles, axis, split_axis=0, concat_axis=0, tiled=True)


def passed_along(x, axis, by):
    length = lax.axis_size(axis)
    pairs = [(i, i + by) for i in range(length) if 0 <= i + by < length]
    return lax.ppermute(x, axis, pairs)


def sent_down(x, axis, radix, step):
    length = lax.axis_size(axis)
    got = []
    for times in range(1, radix):
        pairs = [
            (i + times * step, i)
            for i in range(0, length, radix * step)
            if i + times * step < length
        ]
        if pairs:
            got.append(lax.ppermute(x, axis, pairs))
    return got


def shards(
    token_ids,
    embed_table,
    arriving,
    returning,
    stashed,
    seed_grad,
    expand,
    compress,
    norm_gain,
    w_query,
    key_weight,
    value_weight,
    w_out,
):
    if lax.axis_size("segment") != RADIX**2:
        raise ValueError("segments")
    parts = lax.axis_size("head")
    ticks, span = token_ids.shape
    rank = embed_table.shape[1]
    width = expand.shape[2]
    queries = w_query.shape[2]
    share = span // parts

    def number(tick):
        return jnp.full((1,), tick, jnp.int32)

    gain = norm_gain.reshape(-1, 1, CHUNK)
    payload = shape_of((parts, 2 * share, rank), LOW)
    piece = shape_of((share, rank), LOW)
    wide_piece = shape_of((share, rank), WIDE)
    lot = shape_of((ticks * share, rank), LOW)
    token = shape_of((16, 128), LOW)
    states = [((2, *dims), kind) for dims, kind in state_shapes(span, width, queries)]
    state_outs = tuple(shape_of(*entry) for entry in states)
    work = 2 * span * width * (rank + queries + 2 * HEAD_SIZE)
    lines = pltpu.VMEM((span, rank), LOW)

    picked = call(pick_kernel, shape_of((parts, ticks * share, rank), LOW), [VMEM] * 2, flops=work)(
        token_ids, embed_table
    )
    rows, order = call(sum_kernel, (lot, piece), [VMEM], limit=4)(exchanged(picked, "head"))

    def folding(order):
        return call(
            fold_kernel,
            (
                shape_of((rank, rank), WIDE),
                shape_of((queries, rank), LOW),
                shape_of((width, 2 * HEAD_SIZE), LOW),
            ),
            [VMEM] * 4 + [HBM] * 2,
            [pltpu.SemaphoreType.DMA((2,))],
            flops=2 * (rank + queries) * width * rank,
        )(order, expand[0], compress[0], w_out[0], key_weight[0], value_weight[0])

    def kept_of(tick, order):
        *state, done = call(
            state_kernel,
            (*state_outs, token),
            [SMEM] + [VMEM] * 7,
            flops=work,
        )(number(tick), gain, order, stashed[0], arriving[0], *weights[:3])
        return state, done

    def forward(tick, gathered, out, state):
        out, *state, direct = call(
            forward_kernel,
            (payload, *state_outs, wide_piece),
            [SMEM] + [VMEM] * (9 + STATE),
            [lines],
            flops=work,
            aliases={9 + place: place for place in range(1 + STATE)},
        )(number(tick), gain, basis, gathered, arriving[0], *weights, out, *state)
        return out, state, direct

    def backward(tick, gathered, out, state):
        return call(
            backward_kernel,
            (payload, wide_piece, token),
            [SMEM] + [VMEM] * (10 + STATE),
            [lines, pltpu.VMEM((span, queries), LOW), pltpu.VMEM((width // CHUNK, span, CHUNK), WIDE)],
            flops=work,
            aliases={10: 0},
        )(number(tick), gain, basis, gathered, returning[0], seed_grad, *weights, out, *state)

    got = sent_down(rows, "segment", RADIX, 1)
    basis, folded, kv = folding(order)
    weights = (expand[0], w_query[0], kv, folded)
    state, done = kept_of(0, order)
    rows, spare, out = call(
        functools.partial(join_kernel, len(got)),
        (lot, payload, payload),
        [VMEM] * (2 + len(got)),
        limit=4,
    )(rows, *got, done)
    got = sent_down(rows, "segment", RADIX, RADIX)
    out, direct_back, done = backward(0, spare, out, state)
    rows, tiles = call(
        functools.partial(join_kernel, len(got)), (lot, payload), [VMEM] * (2 + len(got)), limit=4
    )(rows, *got, done)
    out, state, direct = forward(0, exchanged(tiles, "head"), out, state)

    shares = []
    for tick in range(1, ticks):
        sent, sent_back = call(finish_kernel, (piece, piece), [VMEM] * 3, limit=4)(
            exchanged(out, "head"), direct, direct_back
        )
        shares.append((sent, sent_back))
        arrived = passed_along(sent, "segment", 1)
        arrived_back = passed_along(sent_back, "segment", -1)
        state, done = kept_of(tick, sent)
        mixed = call(mix_kernel, payload, [SMEM] + [VMEM] * 5, limit=4)(
            number(tick), arrived, arrived_back, rows, seed_grad, done
        )
        gathered = exchanged(mixed, "head")
        out, state, direct = forward(tick, gathered, out, state)
        out, direct_back, _ = backward(tick, gathered, out, state)
    whole = shape_of((1, ticks, share, rank), LOW)
    return call(
        functools.partial(last_kernel, ticks - 1),
        (whole, whole),
        [VMEM] * (3 + 2 * (ticks - 1)),
        limit=4,
    )(
        exchanged(out, "head"),
        direct,
        direct_back,
        *[pair[0] for pair in shares],
        *[pair[1] for pair in shares],
    )


def solution(mesh):
    return jax.shard_map(
        shards,
        mesh=mesh,
        in_specs=(
            P("groups", None),
            P(("segment", "head"), None),
            P(("groups", "segment"), None, None),
            P(("groups", "segment"), None, None),
            P(("groups", "segment"), None, None, None),
            P("groups", None, None),
            P("segment", None, None),
            P("segment", None, None),
            P("segment", None),
            P("segment", None, "head"),
            P("segment", None, None),
            P("segment", None, None),
            P("segment", "head", None),
        ),
        out_specs=(
            P(("groups", "segment"), None, "head", None),
            P(("groups", "segment"), None, "head", None),
        ),
        check_vma=False,
    )
```

```python
import functools
import math

import jax
import jax.numpy as jnp
from jax import lax
from jax.experimental import pallas as pl
from jax.experimental.pallas import tpu as pltpu
from jax.sharding import PartitionSpec as P

QUERY_HEADS = 32
KEY_VALUE_HEADS = 4
HEAD_SIZE = 128

EPS = 1e-06
CHUNK = 512
LANES = 128
RADIX = 4
LOW = jnp.bfloat16
WIDE = jnp.float32

VMEM = pl.BlockSpec(memory_space=pltpu.VMEM)
SMEM = pl.BlockSpec(memory_space=pltpu.SMEM)
HBM = pl.BlockSpec(memory_space=pltpu.HBM)


def dot(former, latter):
    return jnp.dot(former, latter, preferred_element_type=WIDE)


def dot_back(former, latter):
    return lax.dot_general(former, latter, (((1,), (1,)), ((), ())), preferred_element_type=WIDE)


def dot_turned(former, latter):
    return lax.dot_general(former, latter, (((0,), (0,)), ((), ())), preferred_element_type=WIDE)


def rms_scale(matrix):
    return lax.rsqrt(jnp.mean(matrix * matrix, axis=-1, keepdims=True) + EPS)


def norm_back(upstream_in, grad_hat):
    scaling = rms_scale(upstream_in)
    return scaling * grad_hat - upstream_in * scaling**3 * jnp.mean(
        grad_hat * upstream_in, axis=-1, keepdims=True
    )


def block(place, length):
    at = place * length
    return pl.ds(at if isinstance(at, int) else pl.multiple_of(at, length), length)


STATE = 6


def state_shapes(span, width, queries):
    heads = queries // HEAD_SIZE
    return [
        ((width // CHUNK, span, CHUNK), WIDE),
        ((span, LANES), WIDE),
        ((heads, span, HEAD_SIZE), WIDE),
        ((span, HEAD_SIZE), WIDE),
        ((span, HEAD_SIZE), LOW),
        ((heads, span, span), WIDE),
    ]


def folded_lanes(matrix):
    total = matrix[:, :LANES]
    for at in range(LANES, matrix.shape[1], LANES):
        total += matrix[:, at : at + LANES]
    return total


def spread(coeffs, gain_ref, expand_ref, query_ref, kv_ref, state):
    hidden, scale, queries, keys, values, _ = state
    count = hidden.shape[0]
    span = coeffs.shape[0]
    squares = jnp.zeros((span, LANES), WIDE)
    wide_q = jnp.zeros((span, query_ref.shape[1]), WIDE)
    wide_kv = jnp.zeros((span, kv_ref.shape[1]), WIDE)
    for place in range(count):
        part = dot(coeffs, expand_ref[:, block(place, CHUNK)])
        hidden[place] = part
        squares += folded_lanes(part * part)
        gained = (part * gain_ref[place]).astype(LOW)
        wide_q += dot(gained, query_ref[block(place, CHUNK), :])
        wide_kv += dot(gained, kv_ref[block(place, CHUNK), :])
    mean = jnp.sum(squares, axis=-1, keepdims=True) / (count * CHUNK)
    scaling = jnp.broadcast_to(lax.rsqrt(mean + EPS), scale.shape)
    scale[...] = scaling
    for head in range(queries.shape[0]):
        queries[head] = wide_q[:, head * HEAD_SIZE : (head + 1) * HEAD_SIZE] * scaling
    keys[...] = wide_kv[:, :HEAD_SIZE] * scaling
    values[...] = (wide_kv[:, HEAD_SIZE:] * scaling).astype(LOW)


def hat(matrix):
    return (matrix * rms_scale(matrix)).astype(LOW)


def probabilities(q_hat, k_hat):
    rows = q_hat.shape[0]
    scores = dot_back(q_hat, k_hat) * (1.0 / math.sqrt(HEAD_SIZE))
    column = lax.broadcasted_iota(jnp.int32, (rows, rows), 1)
    row = lax.broadcasted_iota(jnp.int32, (rows, rows), 0)
    weights = jnp.where(column <= row, jnp.exp(scores), 0.0)
    return weights * (1.0 / jnp.sum(weights, axis=-1, keepdims=True))


def attend(folded_ref, state):
    _, _, queries, keys, values, probs = state
    k_hat = hat(keys[...])
    total = None if folded_ref is None else jnp.zeros((keys.shape[0], folded_ref.shape[1]), WIDE)
    for head in range(queries.shape[0]):
        chances = probabilities(hat(queries[head]), k_hat)
        probs[head] = chances
        if folded_ref is not None:
            attended = dot(chances.astype(LOW), values[...]).astype(LOW)
            total += dot(attended, folded_ref[block(head, HEAD_SIZE), :])
    return total


def go_back(grads, gain_ref, expand_ref, query_ref, kv_ref, folded_ref, state, grad_q, weighted_ref):
    hidden, scale, queries, keys, values, probs = state
    count = hidden.shape[0]
    keys_here = keys[...]
    k_hat = hat(keys_here)
    values_here = values[...]
    grad_khat = jnp.zeros(keys_here.shape, WIDE)
    grad_values = jnp.zeros(keys_here.shape, WIDE)
    for head in range(queries.shape[0]):
        upstream = queries[head]
        q_hat = hat(upstream)
        chances = probs[head]
        grad_attended = dot_back(grads, folded_ref[block(head, HEAD_SIZE), :]).astype(LOW)
        grad_chances = dot_back(grad_attended, values_here)
        inner = jnp.sum(grad_chances * chances, axis=-1, keepdims=True)
        grad_scores = chances * (grad_chances - inner) * (1.0 / math.sqrt(HEAD_SIZE))
        grad_scores = grad_scores.astype(LOW)
        grad_q[:, block(head, HEAD_SIZE)] = norm_back(upstream, dot(grad_scores, k_hat)).astype(LOW)
        grad_khat += dot_turned(grad_scores, q_hat)
        grad_values += dot_turned(chances.astype(LOW), grad_attended)
    grad_kv = jnp.concatenate(
        [norm_back(keys_here, grad_khat).astype(LOW), grad_values.astype(LOW)], axis=1
    )
    scaling = scale[:, :1]
    inner = jnp.zeros((keys_here.shape[0], LANES), WIDE)
    for place in range(count):
        grad_normed = dot_back(grad_q[...], query_ref[block(place, CHUNK), :]) + dot_back(
            grad_kv, kv_ref[block(place, CHUNK), :]
        )
        weighted = grad_normed * gain_ref[place]
        weighted_ref[place] = weighted
        inner += folded_lanes(weighted * hidden[place])
    inner = jnp.sum(inner, axis=-1, keepdims=True)
    factor = scaling**3 * (inner / (count * CHUNK))
    total = jnp.zeros(grads.shape, WIDE)
    for place in range(count):
        grad_hidden = scaling * weighted_ref[place] - hidden[place] * factor
        total += dot_back(grad_hidden.astype(LOW), expand_ref[:, block(place, CHUNK)])
    return total


def direct_of(rows, basis_ref, back):
    return lax.dot_general(
        rows.astype(WIDE),
        basis_ref[...],
        (((1,), (1 if back else 0,)), ((), ())),
        precision=lax.Precision.HIGHEST,
        preferred_element_type=WIDE,
    )


def own_rows(ref, share):
    at = lax.axis_index("head") * share
    return ref[pl.ds(pl.multiple_of(at, share), share), :]


def place_in_line():
    return lax.axis_index("segment"), lax.axis_size("segment") - 1


def put_tiles(payload_ref, total, at):
    share = payload_ref.shape[1] // 2
    for place in range(payload_ref.shape[0]):
        payload_ref[place, pl.ds(at, share), :] = total[place * share : (place + 1) * share].astype(
            LOW
        )


def take_tiles(rows_ref, at, other_ref, use_other, out_ref):
    share = rows_ref.shape[1] // 2
    for place in range(rows_ref.shape[0]):
        here = pl.ds(place * share, share)
        out_ref[here, :] = jnp.where(
            use_other, other_ref[here, :], rows_ref[place, pl.ds(at, share), :]
        )


def state_kernel(
    tick_ref, gain_ref, order_ref, stash_ref, other_ref, expand_ref, query_ref, kv_ref, *refs
):
    state = [ref.at[1] for ref in refs[:STATE]]
    segment, last = place_in_line()
    use_other = 2 * (last - segment) == tick_ref[0]
    coeffs = jnp.where(use_other, other_ref[...], stash_ref[tick_ref[0]])
    spread(coeffs, gain_ref, expand_ref, query_ref, kv_ref, state)
    attend(None, state)
    refs[STATE][...] = jnp.zeros(refs[STATE].shape, LOW)


def forward_kernel(
    tick_ref, gain_ref, basis_ref, rows_ref, other_ref, expand_ref, query_ref, kv_ref, folded_ref, *refs
):
    payload_ref, direct_ref, coeffs_ref = refs[1 + STATE], refs[2 + 2 * STATE], refs[3 + 2 * STATE]
    state = [ref.at[0] for ref in refs[2 + STATE : 2 + 2 * STATE]]
    segment, _ = place_in_line()
    use_other = (tick_ref[0] == 0) & (segment != 0)
    take_tiles(rows_ref, 0, other_ref, use_other, coeffs_ref)
    direct_ref[...] = direct_of(own_rows(coeffs_ref, direct_ref.shape[0]), basis_ref, False)
    spread(coeffs_ref[...], gain_ref, expand_ref, query_ref, kv_ref, state)
    put_tiles(payload_ref, attend(folded_ref, state), 0)


def backward_kernel(
    tick_ref,
    gain_ref,
    basis_ref,
    rows_ref,
    returning_ref,
    seed_ref,
    expand_ref,
    query_ref,
    kv_ref,
    folded_ref,
    *refs,
):
    kept = refs[1 : 1 + STATE]
    payload_ref, direct_ref, token_ref, grads_ref, grad_q, weighted = refs[1 + STATE :]
    share = direct_ref.shape[0]
    segment, last = place_in_line()
    first_tick = tick_ref[0] == 0
    for place in range(rows_ref.shape[0]):
        here = pl.ds(place * share, share)
        given = jnp.where(segment == last, seed_ref[0, here, :], returning_ref[here, :])
        grads_ref[here, :] = jnp.where(first_tick, given, rows_ref[place, pl.ds(share, share), :])
    direct_ref[...] = direct_of(own_rows(grads_ref, share), basis_ref, True)
    slot = jnp.where(jnp.logical_not(first_tick) & (segment == last), 0, 1)
    state = [ref.at[slot] for ref in kept]
    total = go_back(
        grads_ref[...], gain_ref, expand_ref, query_ref, kv_ref, folded_ref, state, grad_q, weighted
    )
    put_tiles(payload_ref, total, share)
    token_ref[...] = jnp.zeros(token_ref.shape, LOW)


def pick_kernel(ids_hbm, table_hbm, out_ref, ids_ref, table_ref, hits_ref, sems):
    ids_copy = pltpu.make_async_copy(ids_hbm, ids_ref, sems.at[0])
    table_copy = pltpu.make_async_copy(table_hbm, table_ref, sems.at[1])
    ids_copy.start()
    table_copy.start()
    rows = table_ref.shape[0]
    full = rows // LANES * LANES
    ticks, span = ids_ref.shape
    share = out_ref.shape[1] // ticks
    own = lax.axis_index("segment") * lax.axis_size("head") + lax.axis_index("head")
    lane = lax.broadcasted_iota(jnp.int32, (LANES, LANES), 1).astype(WIDE)
    ids_copy.wait()
    for place in range(ticks * span // LANES):
        tick, at = place * LANES // span, place * LANES % span
        local = (ids_ref[tick : tick + 1, at : at + LANES] - own * rows).astype(WIDE)
        names = jnp.broadcast_to(local, (LANES, LANES)).T
        for first in range(0, rows, LANES):
            hits_ref[pl.ds(place * LANES, LANES), pl.ds(first, LANES)] = jnp.where(
                names == lane + float(first), 1.0, 0.0
            ).astype(LOW)
    table_copy.wait()
    for place in range(ticks * span // LANES):
        tick, at = place * LANES // span, place * LANES % span
        here = pl.ds(place * LANES, LANES)
        found = dot(hits_ref[here, pl.ds(0, full)], table_ref[pl.ds(0, full), :])
        if rows > full:
            found += dot(
                hits_ref[here, pl.ds(full, rows - full)], table_ref[pl.ds(full, rows - full), :]
            )
        for piece in range(LANES // share):
            out_ref[at // share + piece, pl.ds(tick * share, share), :] = found[
                piece * share : (piece + 1) * share
            ].astype(LOW)


def sum_kernel(parts_ref, out_ref, order_ref):
    total = parts_ref[0]
    for place in range(1, parts_ref.shape[0]):
        total += parts_ref[place]
    out_ref[...] = total
    order_ref[...] = total[: order_ref.shape[0]]


def join_kernel(count, rows_ref, *refs):
    got, (token_ref, out_ref, *tiles) = refs[:count], refs[count:]
    total = rows_ref[...]
    for ref in got:
        total += ref[...]
    out_ref[...] = total
    for ref in tiles:
        if len(ref.shape) == 2:
            ref[...] = total[: ref.shape[0]]
            continue
        for place in range(ref.shape[0]):
            ref[place] = total[: ref.shape[1]]


def fold_kernel(
    order_ref, expand_ref, compress_ref, out_weight_ref, key_ref, value_ref, basis_ref, folded_ref, kv_ref, sems
):
    heads_here = out_weight_ref.shape[0] // HEAD_SIZE
    first = lax.axis_index("head") * heads_here * KEY_VALUE_HEADS // QUERY_HEADS * HEAD_SIZE
    here = pl.ds(pl.multiple_of(first, HEAD_SIZE), HEAD_SIZE)
    copies = [
        pltpu.make_async_copy(
            ref.at[:, here], kv_ref.at[:, pl.ds(place * HEAD_SIZE, HEAD_SIZE)], sems.at[place]
        )
        for place, ref in enumerate((key_ref, value_ref))
    ]
    for copy in copies:
        copy.start()
    basis_ref[...] = dot(expand_ref[...], compress_ref[...])
    folded_ref[...] = dot(out_weight_ref[...], compress_ref[...]).astype(folded_ref.dtype)
    for copy in copies:
        copy.wait()


def total_of(parts_ref, at, direct_ref):
    share = direct_ref.shape[0]
    summed = parts_ref[0, pl.ds(at, share), :].astype(WIDE)
    for place in range(1, parts_ref.shape[0]):
        summed += parts_ref[place, pl.ds(at, share), :].astype(WIDE)
    return (summed + direct_ref[...]).astype(LOW)


def finish_kernel(
    parts_ref, direct_ref, direct_back_ref, out_ref, out_back_ref, first_ref, second_ref
):
    ahead = total_of(parts_ref, 0, direct_ref)
    back = total_of(parts_ref, direct_ref.shape[0], direct_back_ref)
    even = lax.axis_index("segment") % 2 == 0
    out_ref[...] = ahead
    out_back_ref[...] = back
    first_ref[...] = jnp.where(even, ahead, back)
    second_ref[...] = jnp.where(even, back, ahead)


def last_kernel(count, parts_ref, direct_ref, direct_back_ref, *refs):
    share = direct_ref.shape[0]
    before, out_ref, out_back_ref = refs[: 2 * count], refs[2 * count], refs[2 * count + 1]
    for place in range(count):
        out_ref[0, place] = before[place][...]
        out_back_ref[0, place] = before[count + place][...]
    out_ref[0, count] = total_of(parts_ref, 0, direct_ref)
    out_back_ref[0, count] = total_of(parts_ref, share, direct_back_ref)


def mix_kernel(tick_ref, first_ref, second_ref, later_ref, seed_ref, token_ref, out_ref):
    share = first_ref.shape[0]
    tick = tick_ref[0]
    segment, last = place_in_line()
    later = later_ref[pl.ds(pl.multiple_of(tick * share, share), share), :]
    even = segment % 2 == 0
    got = jnp.where(even, second_ref[...], first_ref[...])
    got_back = jnp.where(even, first_ref[...], second_ref[...])
    rows = jnp.where(segment == 0, later, got)
    rows_back = jnp.where(segment == last, own_rows(seed_ref.at[tick], share), got_back)
    for place in range(out_ref.shape[0]):
        out_ref[place, pl.ds(0, share), :] = rows
        out_ref[place, pl.ds(share, share), :] = rows_back


def shape_of(dims, kind):
    return jax.ShapeDtypeStruct(dims, kind)


def call(body, outs, specs, scratch=(), flops=0, aliases=None, limit=8):
    kernel = pl.pallas_call(
        body,
        out_shape=outs,
        in_specs=specs,
        out_specs=jax.tree.map(lambda _: VMEM, outs),
        scratch_shapes=list(scratch),
        input_output_aliases=aliases or {},
        cost_estimate=pl.CostEstimate(flops=flops, bytes_accessed=2**20, transcendentals=0),
        compiler_params=pltpu.CompilerParams(vmem_limit_bytes=limit * 2**20),
    )

    def run(*args):
        return kernel(
            *[
                pltpu.with_memory_space_constraint(arg, pltpu.HBM) if spec is HBM else arg
                for spec, arg in zip(specs, args)
            ]
        )

    return run


def exchanged(tiles, axis):
    return lax.all_to_all(tiles, axis, split_axis=0, concat_axis=0, tiled=True)


def swapped(x, axis, start):
    length = lax.axis_size(axis)
    pairs = [(i, i + 1) for i in range(start, length - 1, 2)]
    return lax.ppermute(x, axis, pairs + [(j, i) for i, j in pairs])


def sent_down(x, axis, radix, step):
    length = lax.axis_size(axis)
    got = []
    for times in range(1, radix):
        pairs = [
            (i + times * step, i)
            for i in range(0, length, radix * step)
            if i + times * step < length
        ]
        if pairs:
            got.append(lax.ppermute(x, axis, pairs))
    return got


def shards(
    token_ids,
    embed_table,
    arriving,
    returning,
    stashed,
    seed_grad,
    expand,
    compress,
    norm_gain,
    w_query,
    key_weight,
    value_weight,
    w_out,
):
    if lax.axis_size("segment") != RADIX**2:
        raise ValueError("segments")
    parts = lax.axis_size("head")
    ticks, span = token_ids.shape
    rank = embed_table.shape[1]
    width = expand.shape[2]
    queries = w_query.shape[2]
    share = span // parts

    def number(tick):
        return jnp.full((1,), tick, jnp.int32)

    gain = norm_gain.reshape(-1, 1, CHUNK)
    payload = shape_of((parts, 2 * share, rank), LOW)
    piece = shape_of((share, rank), LOW)
    wide_piece = shape_of((share, rank), WIDE)
    lot = shape_of((ticks * share, rank), LOW)
    token = shape_of((16, 128), LOW)
    states = [((2, *dims), kind) for dims, kind in state_shapes(span, width, queries)]
    state_outs = tuple(shape_of(*entry) for entry in states)
    work = 2 * span * width * (rank + queries + 2 * HEAD_SIZE)
    lines = pltpu.VMEM((span, rank), LOW)

    table_rows = embed_table.shape[0]
    picked = call(
        pick_kernel,
        shape_of((parts, ticks * share, rank), LOW),
        [HBM] * 2,
        [
            pltpu.VMEM(token_ids.shape, jnp.int32),
            pltpu.VMEM(embed_table.shape, LOW),
            pltpu.VMEM((ticks * span, -(-table_rows // LANES) * LANES), LOW),
            pltpu.SemaphoreType.DMA((2,)),
        ],
        flops=work,
    )(token_ids, embed_table)
    rows, order = call(sum_kernel, (lot, piece), [VMEM], limit=4)(exchanged(picked, "head"))

    def folding(order):
        return call(
            fold_kernel,
            (
                shape_of((rank, rank), WIDE),
                shape_of((queries, rank), LOW),
                shape_of((width, 2 * HEAD_SIZE), LOW),
            ),
            [VMEM] * 4 + [HBM] * 2,
            [pltpu.SemaphoreType.DMA((2,))],
            flops=2 * (rank + queries) * width * rank,
        )(order, expand[0], compress[0], w_out[0], key_weight[0], value_weight[0])

    def kept_of(tick, order):
        *state, done = call(
            state_kernel,
            (*state_outs, token),
            [SMEM] + [VMEM] * 7,
            flops=work,
        )(number(tick), gain, order, stashed[0], arriving[0], *weights[:3])
        return state, done

    def forward(tick, gathered, out, state):
        out, *state, direct = call(
            forward_kernel,
            (payload, *state_outs, wide_piece),
            [SMEM] + [VMEM] * (9 + STATE),
            [lines],
            flops=work,
            aliases={9 + place: place for place in range(1 + STATE)},
        )(number(tick), gain, basis, gathered, arriving[0], *weights, out, *state)
        return out, state, direct

    def backward(tick, gathered, out, state):
        return call(
            backward_kernel,
            (payload, wide_piece, token),
            [SMEM] + [VMEM] * (10 + STATE),
            [lines, pltpu.VMEM((span, queries), LOW), pltpu.VMEM((width // CHUNK, span, CHUNK), WIDE)],
            flops=work,
            aliases={10: 0},
        )(number(tick), gain, basis, gathered, returning[0], seed_grad, *weights, out, *state)

    got = sent_down(rows, "segment", RADIX, 1)
    basis, folded, kv = folding(order)
    weights = (expand[0], w_query[0], kv, folded)
    rows, order, spare, out = call(
        functools.partial(join_kernel, len(got)),
        (lot, piece, payload, payload),
        [VMEM] * (2 + len(got)),
        limit=4,
    )(rows, *got, basis)
    got = sent_down(rows, "segment", RADIX, RADIX)
    state, _ = kept_of(0, order)
    out, direct_back, done = backward(0, spare, out, state)
    rows, tiles = call(
        functools.partial(join_kernel, len(got)), (lot, payload), [VMEM] * (2 + len(got)), limit=4
    )(rows, *got, done)
    out, state, direct = forward(0, exchanged(tiles, "head"), out, state)

    shares = []
    for tick in range(1, ticks):
        sent, sent_back, first, second = call(finish_kernel, (piece,) * 4, [VMEM] * 3, limit=4)(
            exchanged(out, "head"), direct, direct_back
        )
        shares.append((sent, sent_back))
        first, second = swapped(first, "segment", 0), swapped(second, "segment", 1)
        state, done = kept_of(tick, sent)
        mixed = call(mix_kernel, payload, [SMEM] + [VMEM] * 5, limit=4)(
            number(tick), first, second, rows, seed_grad, done
        )
        gathered = exchanged(mixed, "head")
        out, state, direct = forward(tick, gathered, out, state)
        out, direct_back, _ = backward(tick, gathered, out, state)
    whole = shape_of((1, ticks, share, rank), LOW)
    return call(
        functools.partial(last_kernel, ticks - 1),
        (whole, whole),
        [VMEM] * (3 + 2 * (ticks - 1)),
        limit=4,
    )(
        exchanged(out, "head"),
        direct,
        direct_back,
        *[pair[0] for pair in shares],
        *[pair[1] for pair in shares],
    )


def solution(mesh):
    return jax.shard_map(
        shards,
        mesh=mesh,
        in_specs=(
            P("groups", None),
            P(("segment", "head"), None),
            P(("groups", "segment"), None, None),
            P(("groups", "segment"), None, None),
            P(("groups", "segment"), None, None, None),
            P("groups", None, None),
            P("segment", None, None),
            P("segment", None, None),
            P("segment", None),
            P("segment", None, "head"),
            P("segment", None, None),
            P("segment", None, None),
            P("segment", "head", None),
        ),
        out_specs=(
            P(("groups", "segment"), None, "head", None),
            P(("groups", "segment"), None, "head", None),
        ),
        check_vma=False,
    )
```

```python
import functools
import math

import jax
import jax.numpy as jnp
from jax import lax
from jax.experimental import pallas as pl
from jax.experimental.pallas import tpu as pltpu
from jax.sharding import PartitionSpec as P

QUERY_HEADS = 32
KEY_VALUE_HEADS = 4
HEAD_SIZE = 128

EPS = 1e-06
CHUNK = 512
LANES = 128
ROUNDS = ((2, 1), (4, 2), (2, 8))
LOW = jnp.bfloat16
WIDE = jnp.float32

VMEM = pl.BlockSpec(memory_space=pltpu.VMEM)
SMEM = pl.BlockSpec(memory_space=pltpu.SMEM)
HBM = pl.BlockSpec(memory_space=pltpu.HBM)


def dot(former, latter):
    return jnp.dot(former, latter, preferred_element_type=WIDE)


def dot_back(former, latter):
    return lax.dot_general(former, latter, (((1,), (1,)), ((), ())), preferred_element_type=WIDE)


def dot_turned(former, latter):
    return lax.dot_general(former, latter, (((0,), (0,)), ((), ())), preferred_element_type=WIDE)


def rms_scale(matrix):
    return lax.rsqrt(jnp.mean(matrix * matrix, axis=-1, keepdims=True) + EPS)


def norm_back(upstream_in, grad_hat):
    scaling = rms_scale(upstream_in)
    return scaling * grad_hat - upstream_in * scaling**3 * jnp.mean(
        grad_hat * upstream_in, axis=-1, keepdims=True
    )


def block(place, length):
    at = place * length
    return pl.ds(at if isinstance(at, int) else pl.multiple_of(at, length), length)


STATE = 6


def state_shapes(span, width, queries):
    heads = queries // HEAD_SIZE
    return [
        ((width // CHUNK, span, CHUNK), WIDE),
        ((span, LANES), WIDE),
        ((heads, span, HEAD_SIZE), WIDE),
        ((span, HEAD_SIZE), WIDE),
        ((span, HEAD_SIZE), LOW),
        ((heads, span, span), WIDE),
    ]


def folded_lanes(matrix):
    total = matrix[:, :LANES]
    for at in range(LANES, matrix.shape[1], LANES):
        total += matrix[:, at : at + LANES]
    return total


def spread(coeffs, gain_ref, expand_ref, query_ref, kv_ref, state):
    hidden, scale, queries, keys, values, _ = state
    count = hidden.shape[0]
    span = coeffs.shape[0]
    squares = jnp.zeros((span, LANES), WIDE)
    wide_q = jnp.zeros((span, query_ref.shape[1]), WIDE)
    wide_kv = jnp.zeros((span, kv_ref.shape[1]), WIDE)
    for place in range(count):
        part = dot(coeffs, expand_ref[:, block(place, CHUNK)])
        hidden[place] = part
        squares += folded_lanes(part * part)
        gained = (part * gain_ref[place]).astype(LOW)
        wide_q += dot(gained, query_ref[block(place, CHUNK), :])
        wide_kv += dot(gained, kv_ref[block(place, CHUNK), :])
    mean = jnp.sum(squares, axis=-1, keepdims=True) / (count * CHUNK)
    scaling = jnp.broadcast_to(lax.rsqrt(mean + EPS), scale.shape)
    scale[...] = scaling
    for head in range(queries.shape[0]):
        queries[head] = wide_q[:, head * HEAD_SIZE : (head + 1) * HEAD_SIZE] * scaling
    keys[...] = wide_kv[:, :HEAD_SIZE] * scaling
    values[...] = (wide_kv[:, HEAD_SIZE:] * scaling).astype(LOW)


def hat(matrix):
    return (matrix * rms_scale(matrix)).astype(LOW)


def probabilities(q_hat, k_hat):
    rows = q_hat.shape[0]
    scores = dot_back(q_hat, k_hat) * (1.0 / math.sqrt(HEAD_SIZE))
    column = lax.broadcasted_iota(jnp.int32, (rows, rows), 1)
    row = lax.broadcasted_iota(jnp.int32, (rows, rows), 0)
    weights = jnp.where(column <= row, jnp.exp(scores), 0.0)
    return weights * (1.0 / jnp.sum(weights, axis=-1, keepdims=True))


def attend(folded_ref, state, attended_ref):
    _, _, queries, keys, values, probs = state
    heads = range(queries.shape[0])
    k_hat = hat(keys[...])
    q_hats = [hat(queries[head]) for head in heads]
    for head in heads:
        probs[head] = probabilities(q_hats[head], k_hat)
    if folded_ref is None:
        return None
    for head in heads:
        attended_ref[:, block(head, HEAD_SIZE)] = dot(
            probs[head].astype(LOW), values[...]
        ).astype(LOW)
    return dot(attended_ref[...], folded_ref[...])


def go_back(grads, gain_ref, expand_ref, query_ref, kv_ref, folded_ref, state, grad_q, weighted_ref):
    hidden, scale, queries, keys, values, probs = state
    count = hidden.shape[0]
    keys_here = keys[...]
    k_hat = hat(keys_here)
    values_here = values[...]
    grad_attended_all = dot_back(grads, folded_ref[...]).astype(LOW)
    grad_khat = jnp.zeros(keys_here.shape[::-1], WIDE)
    grad_values = jnp.zeros(keys_here.shape[::-1], WIDE)
    heads = range(queries.shape[0])
    grad_chances = [
        dot_back(grad_attended_all[:, head * HEAD_SIZE : (head + 1) * HEAD_SIZE], values_here)
        for head in heads
    ]
    for head in heads:
        grad_values += dot_turned(
            grad_attended_all[:, head * HEAD_SIZE : (head + 1) * HEAD_SIZE], probs[head].astype(LOW)
        )
    grad_scores = []
    for head in heads:
        chances = probs[head]
        inner = jnp.sum(grad_chances[head] * chances, axis=-1, keepdims=True)
        scores = chances * (grad_chances[head] - inner) * (1.0 / math.sqrt(HEAD_SIZE))
        grad_scores.append(scores.astype(LOW))
    q_hats = [hat(queries[head]) for head in heads]
    grad_qhats = [dot(grad_scores[head], k_hat) for head in heads]
    for head in heads:
        grad_khat += dot_turned(q_hats[head], grad_scores[head])
    for head in heads:
        grad_q[:, block(head, HEAD_SIZE)] = norm_back(queries[head], grad_qhats[head]).astype(LOW)
    grad_kv = jnp.concatenate(
        [norm_back(keys_here, grad_khat.T).astype(LOW), grad_values.T.astype(LOW)], axis=1
    )
    scaling = scale[:, :1]
    inner = jnp.zeros((keys_here.shape[0], LANES), WIDE)
    for place in range(count):
        grad_normed = dot_back(grad_q[...], query_ref[block(place, CHUNK), :]) + dot_back(
            grad_kv, kv_ref[block(place, CHUNK), :]
        )
        weighted = grad_normed * gain_ref[place]
        weighted_ref[place] = weighted
        inner += folded_lanes(weighted * hidden[place])
    inner = jnp.sum(inner, axis=-1, keepdims=True)
    factor = scaling**3 * (inner / (count * CHUNK))
    total = jnp.zeros(grads.shape, WIDE)
    for place in range(count):
        grad_hidden = scaling * weighted_ref[place] - hidden[place] * factor
        total += dot_back(grad_hidden.astype(LOW), expand_ref[:, block(place, CHUNK)])
    return total


def direct_of(rows, basis_ref, back):
    return lax.dot_general(
        rows.astype(WIDE),
        basis_ref[...],
        (((1,), (1 if back else 0,)), ((), ())),
        precision=lax.Precision.HIGHEST,
        preferred_element_type=WIDE,
    )


def own_rows(ref, share):
    at = lax.axis_index("head") * share
    return ref[pl.ds(pl.multiple_of(at, share), share), :]


def place_in_line():
    return lax.axis_index("segment"), lax.axis_size("segment") - 1


def put_tiles(payload_ref, total, at):
    share = payload_ref.shape[1] // 2
    for place in range(payload_ref.shape[0]):
        payload_ref[place, pl.ds(at, share), :] = total[place * share : (place + 1) * share].astype(
            LOW
        )


def take_tiles(rows_ref, at, other_ref, use_other, out_ref):
    share = rows_ref.shape[1] // 2
    for place in range(rows_ref.shape[0]):
        here = pl.ds(place * share, share)
        out_ref[here, :] = jnp.where(
            use_other, other_ref[here, :], rows_ref[place, pl.ds(at, share), :]
        )


def state_kernel(
    tick_ref, gain_ref, order_ref, stash_ref, other_ref, expand_ref, query_ref, kv_ref, *refs
):
    state = [ref.at[1] for ref in refs[:STATE]]
    segment, last = place_in_line()
    use_other = 2 * (last - segment) == tick_ref[0]
    coeffs = jnp.where(use_other, other_ref[...], stash_ref[tick_ref[0]])
    spread(coeffs, gain_ref, expand_ref, query_ref, kv_ref, state)
    attend(None, state, None)
    refs[STATE][...] = jnp.zeros(refs[STATE].shape, LOW)


def forward_kernel(
    tick_ref, gain_ref, basis_ref, rows_ref, other_ref, expand_ref, query_ref, kv_ref, folded_ref, *refs
):
    payload_ref = refs[1 + STATE]
    direct_ref, coeffs_ref, attended_ref = refs[2 + 2 * STATE :]
    state = [ref.at[0] for ref in refs[2 + STATE : 2 + 2 * STATE]]
    segment, _ = place_in_line()
    use_other = (tick_ref[0] == 0) & (segment != 0)
    take_tiles(rows_ref, 0, other_ref, use_other, coeffs_ref)
    direct_ref[...] = direct_of(own_rows(coeffs_ref, direct_ref.shape[0]), basis_ref, False)
    spread(coeffs_ref[...], gain_ref, expand_ref, query_ref, kv_ref, state)
    put_tiles(payload_ref, attend(folded_ref, state, attended_ref), 0)


def backward_kernel(
    tick_ref,
    gain_ref,
    basis_ref,
    rows_ref,
    returning_ref,
    seed_ref,
    expand_ref,
    query_ref,
    kv_ref,
    folded_ref,
    *refs,
):
    kept = refs[1 : 1 + STATE]
    payload_ref, direct_ref, token_ref, grads_ref, grad_q, weighted = refs[1 + STATE :]
    share = direct_ref.shape[0]
    segment, last = place_in_line()
    first_tick = tick_ref[0] == 0
    for place in range(rows_ref.shape[0]):
        here = pl.ds(place * share, share)
        given = jnp.where(segment == last, seed_ref[0, here, :], returning_ref[here, :])
        grads_ref[here, :] = jnp.where(first_tick, given, rows_ref[place, pl.ds(share, share), :])
    direct_ref[...] = direct_of(own_rows(grads_ref, share), basis_ref, True)
    slot = jnp.where(jnp.logical_not(first_tick) & (segment == last), 0, 1)
    state = [ref.at[slot] for ref in kept]
    total = go_back(
        grads_ref[...], gain_ref, expand_ref, query_ref, kv_ref, folded_ref, state, grad_q, weighted
    )
    put_tiles(payload_ref, total, share)
    token_ref[...] = jnp.zeros(token_ref.shape, LOW)


def pick_kernel(ids_hbm, table_hbm, out_ref, ids_ref, table_ref, hits_ref, sems):
    ids_copy = pltpu.make_async_copy(ids_hbm, ids_ref, sems.at[0])
    table_copy = pltpu.make_async_copy(table_hbm, table_ref, sems.at[1])
    ids_copy.start()
    table_copy.start()
    rows = table_ref.shape[0]
    full = rows // LANES * LANES
    ticks, span = ids_ref.shape
    share = out_ref.shape[1] // ticks
    own = lax.axis_index("segment") * lax.axis_size("head") + lax.axis_index("head")
    lane = lax.broadcasted_iota(jnp.int32, (LANES, LANES), 1).astype(WIDE)
    ids_copy.wait()
    for place in range(ticks * span // LANES):
        tick, at = place * LANES // span, place * LANES % span
        local = (ids_ref[tick : tick + 1, at : at + LANES] - own * rows).astype(WIDE)
        names = jnp.broadcast_to(local, (LANES, LANES)).T
        for first in range(0, rows, LANES):
            hits_ref[pl.ds(place * LANES, LANES), pl.ds(first, LANES)] = jnp.where(
                names == lane + float(first), 1.0, 0.0
            ).astype(LOW)
    table_copy.wait()
    for place in range(ticks * span // LANES):
        tick, at = place * LANES // span, place * LANES % span
        here = pl.ds(place * LANES, LANES)
        found = dot(hits_ref[here, pl.ds(0, full)], table_ref[pl.ds(0, full), :])
        if rows > full:
            found += dot(
                hits_ref[here, pl.ds(full, rows - full)], table_ref[pl.ds(full, rows - full), :]
            )
        for piece in range(LANES // share):
            out_ref[at // share + piece, pl.ds(tick * share, share), :] = found[
                piece * share : (piece + 1) * share
            ].astype(LOW)


def sum_kernel(parts_ref, out_ref, order_ref):
    total = parts_ref[0]
    for place in range(1, parts_ref.shape[0]):
        total += parts_ref[place]
    out_ref[...] = total
    order_ref[...] = total[: order_ref.shape[0]]


def join_kernel(count, rows_ref, *refs):
    got, (token_ref, out_ref, *tiles) = refs[:count], refs[count:]
    total = rows_ref[...]
    for ref in got:
        total += ref[...]
    out_ref[...] = total
    for ref in tiles:
        if len(ref.shape) == 2:
            ref[...] = total[: ref.shape[0]]
            continue
        for place in range(ref.shape[0]):
            ref[place] = total[: ref.shape[1]]


def fold_kernel(
    order_ref, expand_ref, compress_ref, out_weight_ref, key_ref, value_ref, basis_ref, folded_ref, kv_ref, sems
):
    heads_here = out_weight_ref.shape[0] // HEAD_SIZE
    first = lax.axis_index("head") * heads_here * KEY_VALUE_HEADS // QUERY_HEADS * HEAD_SIZE
    here = pl.ds(pl.multiple_of(first, HEAD_SIZE), HEAD_SIZE)
    copies = [
        pltpu.make_async_copy(
            ref.at[:, here], kv_ref.at[:, pl.ds(place * HEAD_SIZE, HEAD_SIZE)], sems.at[place]
        )
        for place, ref in enumerate((key_ref, value_ref))
    ]
    for copy in copies:
        copy.start()
    basis_ref[...] = dot(expand_ref[...], compress_ref[...])
    folded_ref[...] = dot(out_weight_ref[...], compress_ref[...]).astype(folded_ref.dtype)
    for copy in copies:
        copy.wait()


def total_of(parts_ref, at, direct_ref):
    share = direct_ref.shape[0]
    summed = parts_ref[0, pl.ds(at, share), :].astype(WIDE)
    for place in range(1, parts_ref.shape[0]):
        summed += parts_ref[place, pl.ds(at, share), :].astype(WIDE)
    return (summed + direct_ref[...]).astype(LOW)


def finish_kernel(
    parts_ref, direct_ref, direct_back_ref, out_ref, out_back_ref, first_ref, second_ref
):
    ahead = total_of(parts_ref, 0, direct_ref)
    back = total_of(parts_ref, direct_ref.shape[0], direct_back_ref)
    even = lax.axis_index("segment") % 2 == 0
    out_ref[...] = ahead
    out_back_ref[...] = back
    first_ref[...] = jnp.where(even, ahead, back)
    second_ref[...] = jnp.where(even, back, ahead)


def last_kernel(count, parts_ref, direct_ref, direct_back_ref, *refs):
    share = direct_ref.shape[0]
    before, out_ref, out_back_ref = refs[: 2 * count], refs[2 * count], refs[2 * count + 1]
    for place in range(count):
        out_ref[0, place] = before[place][...]
        out_back_ref[0, place] = before[count + place][...]
    out_ref[0, count] = total_of(parts_ref, 0, direct_ref)
    out_back_ref[0, count] = total_of(parts_ref, share, direct_back_ref)


def mix_kernel(tick_ref, first_ref, second_ref, later_ref, seed_ref, token_ref, out_ref):
    share = first_ref.shape[0]
    tick = tick_ref[0]
    segment, last = place_in_line()
    later = later_ref[pl.ds(pl.multiple_of(tick * share, share), share), :]
    even = segment % 2 == 0
    got = jnp.where(even, second_ref[...], first_ref[...])
    got_back = jnp.where(even, first_ref[...], second_ref[...])
    rows = jnp.where(segment == 0, later, got)
    rows_back = jnp.where(segment == last, own_rows(seed_ref.at[tick], share), got_back)
    for place in range(out_ref.shape[0]):
        out_ref[place, pl.ds(0, share), :] = rows
        out_ref[place, pl.ds(share, share), :] = rows_back


def shape_of(dims, kind):
    return jax.ShapeDtypeStruct(dims, kind)


def call(body, outs, specs, scratch=(), flops=0, aliases=None, limit=8):
    kernel = pl.pallas_call(
        body,
        out_shape=outs,
        in_specs=specs,
        out_specs=jax.tree.map(lambda _: VMEM, outs),
        scratch_shapes=list(scratch),
        input_output_aliases=aliases or {},
        cost_estimate=pl.CostEstimate(flops=flops, bytes_accessed=2**20, transcendentals=0),
        compiler_params=pltpu.CompilerParams(vmem_limit_bytes=limit * 2**20),
    )

    def run(*args):
        return kernel(
            *[
                pltpu.with_memory_space_constraint(arg, pltpu.HBM) if spec is HBM else arg
                for spec, arg in zip(specs, args)
            ]
        )

    return run


def exchanged(tiles, axis):
    return lax.all_to_all(tiles, axis, split_axis=0, concat_axis=0, tiled=True)


def swapped(x, axis, start):
    length = lax.axis_size(axis)
    pairs = [(i, i + 1) for i in range(start, length - 1, 2)]
    return lax.ppermute(x, axis, pairs + [(j, i) for i, j in pairs])


def sent_down(x, axis, radix, step):
    length = lax.axis_size(axis)
    got = []
    for times in range(1, radix):
        pairs = [
            (i + times * step, i)
            for i in range(0, length, radix * step)
            if i + times * step < length
        ]
        if pairs:
            got.append(lax.ppermute(x, axis, pairs))
    return got


def shards(
    token_ids,
    embed_table,
    arriving,
    returning,
    stashed,
    seed_grad,
    expand,
    compress,
    norm_gain,
    w_query,
    key_weight,
    value_weight,
    w_out,
):
    if lax.axis_size("segment") != math.prod(radix for radix, _ in ROUNDS):
        raise ValueError("segments")
    parts = lax.axis_size("head")
    ticks, span = token_ids.shape
    rank = embed_table.shape[1]
    width = expand.shape[2]
    queries = w_query.shape[2]
    share = span // parts

    def number(tick):
        return jnp.full((1,), tick, jnp.int32)

    gain = norm_gain.reshape(-1, 1, CHUNK)
    payload = shape_of((parts, 2 * share, rank), LOW)
    piece = shape_of((share, rank), LOW)
    wide_piece = shape_of((share, rank), WIDE)
    lot = shape_of((ticks * share, rank), LOW)
    token = shape_of((16, 128), LOW)
    states = [((2, *dims), kind) for dims, kind in state_shapes(span, width, queries)]
    state_outs = tuple(shape_of(*entry) for entry in states)
    work = 2 * span * width * (rank + queries + 2 * HEAD_SIZE)
    lines = pltpu.VMEM((span, rank), LOW)

    table_rows = embed_table.shape[0]
    picked = call(
        pick_kernel,
        shape_of((parts, ticks * share, rank), LOW),
        [HBM] * 2,
        [
            pltpu.VMEM(token_ids.shape, jnp.int32),
            pltpu.VMEM(embed_table.shape, LOW),
            pltpu.VMEM((ticks * span, -(-table_rows // LANES) * LANES), LOW),
            pltpu.SemaphoreType.DMA((2,)),
        ],
        flops=work,
    )(token_ids, embed_table)
    rows, order = call(sum_kernel, (lot, piece), [VMEM], limit=4)(exchanged(picked, "head"))

    def folding(order):
        return call(
            fold_kernel,
            (
                shape_of((rank, rank), WIDE),
                shape_of((queries, rank), LOW),
                shape_of((width, 2 * HEAD_SIZE), LOW),
            ),
            [VMEM] * 4 + [HBM] * 2,
            [pltpu.SemaphoreType.DMA((2,))],
            flops=2 * (rank + queries) * width * rank,
        )(order, expand[0], compress[0], w_out[0], key_weight[0], value_weight[0])

    def kept_of(tick, order):
        *state, done = call(
            state_kernel,
            (*state_outs, token),
            [SMEM] + [VMEM] * 7,
            flops=work,
        )(number(tick), gain, order, stashed[0], arriving[0], *weights[:3])
        return state, done

    def forward(tick, gathered, out, state):
        out, *state, direct = call(
            forward_kernel,
            (payload, *state_outs, wide_piece),
            [SMEM] + [VMEM] * (9 + STATE),
            [lines, pltpu.VMEM((span, queries), LOW)],
            flops=work,
            aliases={9 + place: place for place in range(1 + STATE)},
        )(number(tick), gain, basis, gathered, arriving[0], *weights, out, *state)
        return out, state, direct

    def backward(tick, gathered, out, state):
        return call(
            backward_kernel,
            (payload, wide_piece, token),
            [SMEM] + [VMEM] * (10 + STATE),
            [lines, pltpu.VMEM((span, queries), LOW), pltpu.VMEM((width // CHUNK, span, CHUNK), WIDE)],
            flops=work,
            aliases={10: 0},
        )(number(tick), gain, basis, gathered, returning[0], seed_grad, *weights, out, *state)

    def joined(outs, rows, got, done):
        return call(
            functools.partial(join_kernel, len(got)), outs, [VMEM] * (2 + len(got)), limit=4
        )(rows, *got, done)

    got = sent_down(rows, "segment", *ROUNDS[0])
    basis, folded, kv = folding(order)
    weights = (expand[0], w_query[0], kv, folded)
    rows, order = joined((lot, piece), rows, got, basis)
    got = sent_down(rows, "segment", *ROUNDS[1])
    state, done = kept_of(0, order)
    rows, spare, out = joined((lot, payload, payload), rows, got, done)
    got = sent_down(rows, "segment", *ROUNDS[2])
    out, direct_back, done = backward(0, spare, out, state)
    rows, tiles = joined((lot, payload), rows, got, done)
    out, state, direct = forward(0, exchanged(tiles, "head"), out, state)

    shares = []
    for tick in range(1, ticks):
        sent, sent_back, first, second = call(finish_kernel, (piece,) * 4, [VMEM] * 3, limit=4)(
            exchanged(out, "head"), direct, direct_back
        )
        shares.append((sent, sent_back))
        first, second = swapped(first, "segment", 0), swapped(second, "segment", 1)
        state, done = kept_of(tick, sent)
        mixed = call(mix_kernel, payload, [SMEM] + [VMEM] * 5, limit=4)(
            number(tick), first, second, rows, seed_grad, done
        )
        gathered = exchanged(mixed, "head")
        out, state, direct = forward(tick, gathered, out, state)
        out, direct_back, _ = backward(tick, gathered, out, state)
    whole = shape_of((1, ticks, share, rank), LOW)
    return call(
        functools.partial(last_kernel, ticks - 1),
        (whole, whole),
        [VMEM] * (3 + 2 * (ticks - 1)),
        limit=4,
    )(
        exchanged(out, "head"),
        direct,
        direct_back,
        *[pair[0] for pair in shares],
        *[pair[1] for pair in shares],
    )


def solution(mesh):
    return jax.shard_map(
        shards,
        mesh=mesh,
        in_specs=(
            P("groups", None),
            P(("segment", "head"), None),
            P(("groups", "segment"), None, None),
            P(("groups", "segment"), None, None),
            P(("groups", "segment"), None, None, None),
            P("groups", None, None),
            P("segment", None, None),
            P("segment", None, None),
            P("segment", None),
            P("segment", None, "head"),
            P("segment", None, None),
            P("segment", None, None),
            P("segment", "head", None),
        ),
        out_specs=(
            P(("groups", "segment"), None, "head", None),
            P(("groups", "segment"), None, "head", None),
        ),
        check_vma=False,
    )
```
